512 devices in a mesh: grp: 4 (over x), dom: 128 (over z, y, core).
Axes of the slice: x: 4, y: 4, z: 16, core: 2. Of those that a mesh axis runs over, the one named last changes fastest.
Arguments:
- node_state: float32 [65536, 6, 128], P(('grp', 'dom')), may hold values from -6 to 6
- node_dest: int32 [65536], P(('grp', 'dom')), may hold values from 0 to 127, as said below
- seg_nodes: float32 [6, 262144], P(None, ('grp', 'dom')), may hold values from -6 to 6
- seg_conn: int32 [3, 524288], P(None, ('grp', 'dom')), may hold values from 0 to 511
- pair_seg: int32 [512, 4, 32], P(('grp', 'dom')), may hold values from 0 to 7
- pair_slot: int32 [512, 4, 32], P(('grp', 'dom')), may hold values from 0 to 255, as said below
Outputs:
- node_force: float32 [65536, 3, 128], P(('grp', 'dom'))
The draws below stay inside these ranges and needn't reach their ends.
Inputs may be any that keep to these rules, and one draw needn't show every extreme that they name: `node_dest`: at most 2 blocks of one device name the same contact domain; in every grp row one contact domain receives exactly 2 blocks from every device of that row; every device sends at least one block to the contact domain of its own dom index. `pair_slot`: every entry names a slot d * 2 + k that holds a block: device (r, d) sends more than k blocks to the contact domain.
All inputs are finite; a program needn't handle non-finite values.
Results may differ from the reference program's by a relative error of at most 0.00023.
Values sent between devices are 32-bit elements; how exact they have to be, the bound alone decides.
No kernel may reach another device: no remote copies, remote signals or barrier semaphores. Data moves between devices by JAX's collectives and lax.ppermute only.
A program may use at most 64 MiB of HBM per device.

```python
import jax
import jax.numpy as jnp
from jax import lax

NODE_BLK = 128
SEG_BLK = 128
NB_DEV = 128
SB_DEV = 8
PAIR_GRP = 32
SN_DEV = 512
CAP = 2
ALL_BLK = 65536
ALL_SEG = 524288
ALL_SN = 262144
N_GRP = 4
N_DOM = 128


def route_tables(key):
    base = jax.random.fold_in(key, 4242)
    key_perm, key_hot, key_shuffle, key_pick = jax.random.split(base, 4)
    senders = N_GRP * N_DOM
    tokens = N_DOM * CAP
    hot_dom = jax.random.randint(key_hot, (N_GRP,), 0, N_DOM)
    perms = jax.vmap(lambda sub_key: jax.random.permutation(sub_key, tokens))(jax.random.split(key_perm, senders))
    sender_ids = jnp.arange(senders, dtype=jnp.int32)
    row_ids = sender_ids // N_DOM
    own_dom = sender_ids % N_DOM
    token_dom = perms // CAP
    is_hot = token_dom == hot_dom[row_ids][:, None]
    is_own = (token_dom == own_dom[:, None]) & (perms % CAP == 0) & jnp.logical_not(is_hot)
    priority = jnp.where(is_hot, 0, jnp.where(is_own, 1, 2))
    score = priority * tokens + jnp.arange(tokens, dtype=jnp.int32)[None, :]
    order_ids = jnp.argsort(score, axis=1)
    chosen = jnp.take_along_axis(perms, order_ids, axis=1)[:, :NB_DEV] // CAP
    shuffles = jax.vmap(lambda sub_key: jax.random.permutation(sub_key, NB_DEV))(jax.random.split(key_shuffle, senders))
    target_dom = jnp.take_along_axis(chosen, shuffles, axis=1).astype(jnp.int32)
    counts = jnp.sum((target_dom[:, :, None] == jnp.arange(N_DOM, dtype=jnp.int32)[None, None, :]).astype(jnp.int32), axis=1)
    per_row = counts.reshape(N_GRP, N_DOM, N_DOM)
    live = jnp.arange(CAP, dtype=jnp.int32)[None, None, None, :] < per_row[:, :, :, None]
    live = jnp.transpose(live, (0, 2, 1, 3)).reshape(N_GRP, N_DOM, N_DOM * CAP).astype(jnp.int32)
    running = jnp.cumsum(live, axis=2)
    total_live = running[:, :, -1]
    raw_pick = jax.random.randint(key_pick, (N_GRP, N_DOM, N_GRP, PAIR_GRP), 0, 1 << 30)
    limit = jnp.transpose(total_live, (1, 0))
    chosen_rank = raw_pick % limit[None, :, :, None]
    run_table = jnp.transpose(running, (1, 0, 2))
    slot_ids = jnp.sum((run_table[None, :, :, None, :] <= chosen_rank[..., None]).astype(jnp.int32), axis=-1)
    return (target_dom.reshape(-1), slot_ids.reshape(N_GRP * N_DOM, N_GRP, PAIR_GRP).astype(jnp.int32))


def draw_node_dest(key, part):
    return route_tables(key)[0]


def draw_pair_slot(key, part):
    return route_tables(key)[1]


def with_ends(drawn, stream_key, smallest, largest):
    dims = drawn.shape
    index_at = [jax.random.randint(jax.random.fold_in(stream_key, axis), (), 0, dims[axis]) for axis in range(len(dims))]
    drawn = drawn.at[tuple(index_at)].set(smallest)
    longest = dims.index(max(dims))
    index_at[longest] = (index_at[longest] + 1) % dims[longest]
    return drawn.at[tuple(index_at)].set(largest)


def level_of(stream_key, shape, pieces, smallest, largest):
    def one(dim, blocks):
        steps = jax.random.uniform(jax.random.fold_in(jax.random.fold_in(stream_key, 6), dim), (blocks,), jnp.float32, smallest / len(pieces), largest / len(pieces))
        return jnp.repeat(jnp.exp(steps), shape[dim] // blocks).reshape((-1,) + (1,) * (len(shape) - dim - 1))

    level = one(*pieces[0])
    for cut in pieces[1:]:
        level = level * one(*cut)
    return level


def normal_values(own_key, dims, scale, most, cuts=(), kind=jnp.bfloat16):
    values = jax.random.normal(own_key, dims, jnp.float32) * scale
    if len(cuts) > 0:
        values = level_of(own_key, dims, cuts, -0.22, 0.18) * values
    return jnp.clip(values, min=-most, max=most).astype(kind)


def setup_inputs(seed: int = 0) -> dict:
    arg_keys = jax.random.split(jax.random.key(seed), 7)
    node_state = normal_values(arg_keys[0], (ALL_BLK, 6, NODE_BLK), 1.0, 6.0, ((0, 512),), jnp.float32)
    node_dest = draw_node_dest(jax.random.fold_in(arg_keys[6], 71), 0)
    seg_nodes = normal_values(arg_keys[2], (6, ALL_SN), 1.0, 6.0, ((1, 512),), jnp.float32)
    seg_conn = with_ends(jax.random.randint(arg_keys[3], (3, ALL_SEG), 0, SN_DEV), jax.random.fold_in(arg_keys[3], 1), 0, SN_DEV - 1).astype(jnp.int32)
    pair_seg = with_ends(jax.random.randint(arg_keys[4], (N_GRP * N_DOM, N_GRP, PAIR_GRP), 0, SB_DEV), jax.random.fold_in(arg_keys[4], 1), 0, SB_DEV - 1).astype(jnp.int32)
    pair_slot = draw_pair_slot(jax.random.fold_in(arg_keys[6], 71), 0)
    return dict(node_state=node_state, node_dest=node_dest, seg_nodes=seg_nodes, seg_conn=seg_conn, pair_seg=pair_seg, pair_slot=pair_slot)


time_step = 0.5
stiffness = 0.5
radius_sq = 0.5


def seg_geometry(corners):
    corner_a = corners[:, 0]
    corner_b = corners[:, 1]
    corner_c = corners[:, 2]
    edge_one = corner_b[0:3] - corner_a[0:3]
    edge_two = corner_c[0:3] - corner_a[0:3]
    normal = 0.5 * jnp.stack([
        edge_one[1] * edge_two[2] - edge_one[2] * edge_two[1],
        edge_one[2] * edge_two[0] - edge_one[0] * edge_two[2],
        edge_one[0] * edge_two[1] - edge_one[1] * edge_two[0]])
    centre = (corner_a[0:3] + corner_b[0:3] + corner_c[0:3]) / 3.0
    motion = (corner_a[3:6] + corner_b[3:6] + corner_c[3:6]) / 3.0
    return jnp.concatenate([normal, centre, motion], axis=0)


def tile_force(node_rows, geometry):
    clearance = jnp.zeros((geometry.shape[1], node_rows.shape[1]), jnp.float32)
    distance = jnp.zeros((geometry.shape[1], node_rows.shape[1]), jnp.float32)
    for axis_id in range(3):
        offset = node_rows[axis_id][None, :] - geometry[3 + axis_id][:, None]
        drift = node_rows[3 + axis_id][None, :] - geometry[6 + axis_id][:, None]
        clearance = clearance + geometry[axis_id][:, None] * (offset + time_step * drift)
        distance = distance + offset * offset
    pressure = stiffness * jnp.exp(-distance / radius_sq) * jnp.maximum(-clearance, 0.0)
    return jnp.dot(geometry[0:3], pressure, precision=lax.Precision.HIGHEST, preferred_element_type=jnp.float32)


def reference(node_state, node_dest, seg_nodes, seg_conn, pair_seg, pair_slot):
    devices = N_GRP * N_DOM
    seg_owner = jnp.arange(seg_conn.shape[1], dtype=jnp.int32) // (SB_DEV * SEG_BLK)
    corners = jnp.take(seg_nodes, seg_conn + (seg_owner * SN_DEV)[None, :], axis=1)
    geometry = seg_geometry(corners)
    geo_blocks = jnp.transpose(geometry.reshape(9, devices * SB_DEV, SEG_BLK), (1, 0, 2))
    target_dom = node_dest.reshape(devices, NB_DEV)
    order_ids = jnp.arange(NB_DEV, dtype=jnp.int32)
    earlier = order_ids[None, :] < order_ids[:, None]
    same_dom = target_dom[:, :, None] == target_dom[:, None, :]
    slot_rank = jnp.sum((same_dom & earlier[None, :, :]).astype(jnp.int32), axis=2)
    device_ids = jnp.arange(devices, dtype=jnp.int32)
    contact_dom = (device_ids % N_DOM)[:, None, None]
    sender = jnp.arange(N_GRP, dtype=jnp.int32)[None, :, None] * N_DOM + pair_slot // CAP
    wanted_rank = pair_slot % CAP
    matching = (target_dom[sender] == contact_dom[..., None]) & (slot_rank[sender] == wanted_rank[..., None])
    local_block = jnp.sum(jnp.where(matching, order_ids, 0), axis=3)
    block_ids = (sender * NB_DEV + local_block).astype(jnp.int32)
    seg_ids = (device_ids[:, None, None] * SB_DEV + pair_seg).astype(jnp.int32)

    def device_forces(device_idx):
        node_rows = jnp.take(node_state, block_ids[device_idx].reshape(-1), axis=0)
        seg_rows = jnp.take(geo_blocks, seg_ids[device_idx].reshape(-1), axis=0)
        return jax.vmap(tile_force)(node_rows, seg_rows)

    forces = lax.map(device_forces, device_ids)
    return jax.ops.segment_sum(forces.reshape(-1, 3, NODE_BLK), block_ids.reshape(-1), num_segments=devices * NB_DEV)
```

```python
import functools
import math

import jax
import jax.numpy as jnp
from jax import lax
from jax.experimental import pallas as pl
from jax.experimental.pallas import tpu as pltpu
from jax.sharding import Mesh
from jax.sharding import PartitionSpec as P

BLK = 128
COPIES = 4
TIME_STEP = 0.5
STIFFNESS = 0.5
RADIUS_SQ = 0.5
SCALE = math.sqrt(math.log2(math.e) / RADIUS_SQ)
GRP_DOM = ("grp", "zh", "zl", "y", "core")
NEAR = ("zl", "y", "core")
VMEM = pl.BlockSpec(memory_space=pltpu.VMEM)
SMEM = pl.BlockSpec(memory_space=pltpu.SMEM)


def lane_pick(row, index):
    return jnp.take_along_axis(row, index, axis=1, mode="promise_in_bounds")


def geometry_kernel(nodes_ref, conn_ref, seg_ref, slot_ref, out_ref):
    blocks = conn_ref.shape[1] // BLK
    parts = nodes_ref.shape[1] // BLK
    index = [
        jnp.concatenate([conn_ref[k : k + 1, b * BLK : (b + 1) * BLK] for b in range(blocks)], axis=0)
        for k in range(3)
    ]
    lanes = [i & (BLK - 1) for i in index]
    part = [i >> 7 for i in index]
    corner = [[None] * 6 for _ in range(3)]
    for comp in range(6):
        for p in range(parts):
            row = jnp.broadcast_to(nodes_ref[comp : comp + 1, p * BLK : (p + 1) * BLK], (blocks, BLK))
            for k in range(3):
                got = lane_pick(row, lanes[k])
                corner[k][comp] = got if p == 0 else jnp.where(part[k] == p, got, corner[k][comp])
    a, b, c = corner
    e = [b[i] - a[i] for i in range(3)]
    f = [c[i] - a[i] for i in range(3)]
    n = [
        0.5 * (e[1] * f[2] - e[2] * f[1]),
        0.5 * (e[2] * f[0] - e[0] * f[2]),
        0.5 * (e[0] * f[1] - e[1] * f[0]),
    ]
    m = [(a[i] + b[i] + c[i]) / 3.0 for i in range(3)]
    u = [(a[i] + b[i] + c[i]) / 3.0 for i in range(3, 6)]
    s = sum(n[i] * (m[i] + TIME_STEP * u[i]) for i in range(3))
    rows = n + [m[i] * SCALE for i in range(3)] + [s]
    tables = jnp.concatenate(
        [slot_ref[...], seg_ref[...], jnp.zeros((blocks - 2, BLK), jnp.int32)], axis=0
    ).astype(jnp.float32)
    for copy in range(out_ref.shape[0]):
        for i, row in enumerate(rows + [tables]):
            out_ref[copy, :, i, :] = row


def three_parts(x):
    high = x.astype(jnp.bfloat16)
    rest = x - high.astype(jnp.float32)
    mid = rest.astype(jnp.bfloat16)
    low = (rest - mid.astype(jnp.float32)).astype(jnp.bfloat16)
    return high, mid, low


def exact_dot(onehot, x):
    return sum(jnp.dot(onehot, part, preferred_element_type=jnp.float32) for part in three_parts(x))


def place_kernel(copies, near, dest_ref, nodes_ref, out_ref, pick_ref):
    blocks = dest_ref.shape[1]
    slots = near * copies * 2
    across = jnp.broadcast_to(dest_ref[...].astype(jnp.float32), (blocks, blocks))
    down = across.T
    i = lax.broadcasted_iota(jnp.int32, (blocks, blocks), 0)
    j = lax.broadcasted_iota(jnp.int32, (blocks, blocks), 1)
    same = across == down

    def slot_of(dest, rank):
        dest = dest.astype(jnp.int32)
        return ((dest & (near - 1)) * copies + lax.div(dest, near)) * 2 + rank.astype(jnp.int32)

    rank_row = jnp.sum(jnp.where(same & (i < j), 1.0, 0.0), axis=0, keepdims=True)
    slot_row = slot_of(dest_ref[...], rank_row)
    onehot = (lax.broadcasted_iota(jnp.int32, (slots, blocks), 0) == slot_row).astype(jnp.float32).astype(jnp.bfloat16)
    rank_col = jnp.sum(jnp.where(same & (j < i), 1.0, 0.0), axis=1, keepdims=True)
    slot_col = slot_of(down[:, 0:1], rank_col)
    pick_ref[...] = (
        (lax.broadcasted_iota(jnp.int32, (blocks, slots), 1) == slot_col).astype(jnp.float32).astype(jnp.bfloat16)
    )
    for comp in range(6):
        x = nodes_ref[comp % 3]
        row = x * SCALE if comp < 3 else x + TIME_STEP * nodes_ref[comp]
        out_ref[:, comp] = exact_dot(onehot, row).reshape(near, copies * 2, BLK)


def force_kernel(codes_ref, geo_ref, nodes_ref, out_ref, turned, todo):
    near, _, slots, _ = out_ref.shape
    pairs = codes_ref.shape[0]
    for t in range(turned.shape[0]):
        turned[t] = geo_ref[t * BLK : (t + 1) * BLK, :].T
    out_ref[...] = jnp.zeros_like(out_ref)

    def keep(k, count):
        code = codes_ref[k]
        todo[count] = code
        return count + jnp.where(code >= 0, 1, 0)

    count = lax.fori_loop(0, pairs, keep, jnp.int32(0), unroll=8)

    def pair(k, _):
        code = todo[k]
        source = code & 63
        slot = (code >> 6) & 31
        block = code >> 11
        tile = block >> 4
        lane = (block & 15) * 8
        row = [nodes_ref[source, comp, pl.ds(slot, 1), :] for comp in range(6)]
        x = [jnp.broadcast_to(r, (8, BLK)) for r in row]
        index = [jnp.full((8, BLK), lane + q, jnp.int32) for q in range(7)]
        force = [jnp.zeros((8, BLK), jnp.float32)] * 3
        for g in range(BLK // 8):
            seg = turned[tile, g * 8 : (g + 1) * 8, :]
            q = [lane_pick(seg, index[i]) for i in range(7)]
            d = [x[i] - q[3 + i] for i in range(3)]
            close = q[6] - (q[0] * x[3] + q[1] * x[4] + q[2] * x[5])
            far = d[0] * d[0] + d[1] * d[1] + d[2] * d[2]
            pressure = jnp.exp2(-far) * jnp.maximum(close, 0.0)
            force = [force[i] + q[i] * pressure for i in range(3)]
        for i in range(3):
            at = (source, i, pl.ds(slot, 1), slice(None))
            out_ref[at] = out_ref[at] + jnp.sum(force[i], axis=0, keepdims=True)
        return 0

    lax.fori_loop(0, count, pair, 0)


def pick_kernel(pick_ref, back_ref, out_ref):
    for comp in range(3):
        rows = back_ref[:, comp].reshape(pick_ref.shape[1], BLK)
        out_ref[comp] = STIFFNESS * exact_dot(pick_ref[...], rows)


def f32(*shape):
    return jax.ShapeDtypeStruct(shape, jnp.float32)


def shards(node_state, node_dest, seg_nodes, seg_conn, pair_seg, pair_slot):
    groups = lax.axis_size("grp")
    copies = lax.axis_size("zh")
    near = lax.axis_size(NEAR)
    blocks = node_state.shape[0]
    seg_blocks = seg_conn.shape[1] // BLK
    per_group = pair_seg.shape[2]
    slots = copies * 2

    geometry = pl.pallas_call(
        geometry_kernel, out_shape=f32(copies, seg_blocks, 8, BLK), in_specs=[VMEM] * 4, out_specs=VMEM
    )(seg_nodes, seg_conn, pair_seg.reshape(1, BLK), pair_slot.reshape(1, BLK))
    geometry = geometry.reshape(copies, seg_blocks * 8, BLK)
    geometry = lax.all_to_all(geometry, "zh", split_axis=0, concat_axis=0, tiled=True)
    geometry = jnp.broadcast_to(
        geometry.reshape(1, copies * seg_blocks * 8, BLK), (groups, copies * seg_blocks * 8, BLK)
    )
    geometry = lax.all_to_all(geometry, "grp", split_axis=0, concat_axis=0, tiled=True)

    outgoing, pick = pl.pallas_call(
        functools.partial(place_kernel, copies, near),
        out_shape=(f32(near, 6, slots, BLK), jax.ShapeDtypeStruct((blocks, near * slots), jnp.bfloat16)),
        in_specs=[VMEM] * 2,
        out_specs=[VMEM] * 2,
    )(node_dest.reshape(1, blocks), jnp.transpose(node_state, (1, 0, 2)))
    received = lax.all_to_all(
        outgoing.reshape(near, 6 * slots, BLK), NEAR, split_axis=0, concat_axis=0, tiled=True
    ).reshape(near, 6, slots, BLK)

    tables = geometry.reshape(groups, copies, seg_blocks, 8, BLK)[:, :, 0:2, 7, :].reshape(
        groups * copies, 2, groups, per_group
    )
    tables = lax.dynamic_index_in_dim(tables, lax.axis_index("grp"), axis=2, keepdims=False).astype(jnp.int32)
    slot, seg = tables[:, 0], tables[:, 1]
    owner = jnp.arange(groups * copies, dtype=jnp.int32)[:, None]
    source = slot // 2
    place = (owner % copies) * 2 + slot % 2
    block = owner * seg_blocks + seg
    codes = (source % near) + place * 64 + block * 2048
    codes = jnp.where(source // near == lax.axis_index("zh"), codes, -1).reshape(-1)

    tiles = groups * copies * seg_blocks * 8 // BLK
    forces = pl.pallas_call(
        force_kernel,
        out_shape=f32(near, 3, slots, BLK),
        in_specs=[SMEM, VMEM, VMEM],
        out_specs=VMEM,
        scratch_shapes=[
            pltpu.VMEM((tiles, BLK, BLK), jnp.float32),
            pltpu.SMEM((codes.shape[0] + 1,), jnp.int32),
        ],
    )(codes, geometry.reshape(tiles * BLK, BLK), received)
    back = lax.all_to_all(
        forces.reshape(near, 3 * slots, BLK), NEAR, split_axis=0, concat_axis=0, tiled=True
    ).reshape(near, 3, slots, BLK)
    out = pl.pallas_call(pick_kernel, out_shape=f32(3, blocks, BLK), in_specs=[VMEM] * 2, out_specs=VMEM)(pick, back)
    return jnp.transpose(out, (1, 0, 2))


def solution(mesh):
    groups = mesh.shape["grp"]
    split = Mesh(mesh.devices.reshape(groups, COPIES, 16 // COPIES, 4, 2), GRP_DOM)
    placed = (
        P(GRP_DOM, None, None),
        P(GRP_DOM),
        P(None, GRP_DOM),
        P(None, GRP_DOM),
        P(GRP_DOM, None, None),
        P(GRP_DOM, None, None),
    )
    return jax.shard_map(
        shards, mesh=split, in_specs=placed, out_specs=P(GRP_DOM, None, None), check_vma=False
    )
```

```python
import functools
import math

import jax
import jax.numpy as jnp
from jax import lax
from jax.experimental import pallas as pl
from jax.experimental.pallas import tpu as pltpu
from jax.sharding import Mesh
from jax.sharding import PartitionSpec as P


BLK = 128
COPIES = 4
TIME_STEP = 0.5
STIFFNESS = 0.5
RADIUS_SQ = 0.5
SCALE = math.sqrt(math.log2(math.e) / RADIUS_SQ)
GRP_DOM = ("grp", "zh", "zl", "y", "core")
NEAR = ("zl", "y", "core")
VMEM = pl.BlockSpec(memory_space=pltpu.VMEM)
SMEM = pl.BlockSpec(memory_space=pltpu.SMEM)
TOGETHER = 4
NOBODY = 256


def room(mib):
    return pltpu.CompilerParams(vmem_limit_bytes=mib << 20)


def lane_pick(row, index):
    return jnp.take_along_axis(row, index, axis=1, mode="promise_in_bounds")


def geometry_kernel(nodes_ref, conn_ref, seg_ref, slot_ref, out_ref):
    blocks = conn_ref.shape[1] // BLK
    parts = nodes_ref.shape[1] // BLK
    index = [
        jnp.concatenate([conn_ref[k : k + 1, b * BLK : (b + 1) * BLK] for b in range(blocks)], axis=0)
        for k in range(3)
    ]
    lanes = [i & (BLK - 1) for i in index]
    part = [i >> 7 for i in index]
    corner = [[None] * 6 for _ in range(3)]
    for comp in range(6):
        for p in range(parts):
            row = jnp.broadcast_to(nodes_ref[comp : comp + 1, p * BLK : (p + 1) * BLK], (blocks, BLK))
            for k in range(3):
                got = lane_pick(row, lanes[k])
                corner[k][comp] = got if p == 0 else jnp.where(part[k] == p, got, corner[k][comp])
    a, b, c = corner
    e = [b[i] - a[i] for i in range(3)]
    f = [c[i] - a[i] for i in range(3)]
    n = [
        0.5 * (e[1] * f[2] - e[2] * f[1]),
        0.5 * (e[2] * f[0] - e[0] * f[2]),
        0.5 * (e[0] * f[1] - e[1] * f[0]),
    ]
    m = [(a[i] + b[i] + c[i]) / 3.0 for i in range(3)]
    u = [(a[i] + b[i] + c[i]) / 3.0 for i in range(3, 6)]
    s = sum(n[i] * (m[i] + TIME_STEP * u[i]) for i in range(3))
    rows = [m[i] * (2.0 * SCALE) for i in range(3)] + [-v for v in n] + [s]
    groups, each = slot_ref.shape[1:]
    tables = jnp.concatenate([slot_ref[0], seg_ref[0]], axis=0).astype(jnp.float32)
    tables = jnp.concatenate([tables, jnp.zeros((2 * groups, BLK - each), jnp.float32)], axis=1)
    for i, row in enumerate(rows + [tables]):
        out_ref[:, i, :] = row


def three_parts(x):
    high = x.astype(jnp.bfloat16)
    rest = x - high.astype(jnp.float32)
    mid = rest.astype(jnp.bfloat16)
    low = (rest - mid.astype(jnp.float32)).astype(jnp.bfloat16)
    return high, mid, low


def exact_dot(onehot, x):
    return sum(jnp.dot(onehot, part, preferred_element_type=jnp.float32) for part in three_parts(x))


def place_kernel(copies, near, dest_ref, nodes_ref, out_ref, pick_ref):
    blocks = dest_ref.shape[1]
    slots = near * copies * 2
    across = jnp.broadcast_to(dest_ref[...].astype(jnp.float32), (blocks, blocks))
    down = across.T
    i = lax.broadcasted_iota(jnp.int32, (blocks, blocks), 0)
    j = lax.broadcasted_iota(jnp.int32, (blocks, blocks), 1)
    same = across == down

    def slot_of(dest, rank):
        dest = dest.astype(jnp.int32)
        return ((dest & (near - 1)) * copies + lax.div(dest, near)) * 2 + rank.astype(jnp.int32)

    rank_row = jnp.sum(jnp.where(same & (i < j), 1.0, 0.0), axis=0, keepdims=True)
    slot_row = slot_of(dest_ref[...], rank_row)
    onehot = (lax.broadcasted_iota(jnp.int32, (slots, blocks), 0) == slot_row).astype(jnp.float32).astype(jnp.bfloat16)
    rank_col = jnp.sum(jnp.where(same & (j < i), 1.0, 0.0), axis=1, keepdims=True)
    slot_col = slot_of(down[:, 0:1], rank_col)
    pick_ref[...] = (
        (lax.broadcasted_iota(jnp.int32, (blocks, slots), 1) == slot_col).astype(jnp.float32).astype(jnp.bfloat16)
    )
    for comp in range(6):
        x = nodes_ref[comp % 3]
        row = x * SCALE if comp < 3 else x + TIME_STEP * nodes_ref[comp]
        out_ref[:, comp] = exact_dot(onehot, row).reshape(near, copies * 2, BLK)


def start_kernel(copies, near, dest_ref, nodes_ref, corners_ref, conn_ref, seg_ref, slot_ref, out_ref, pick_ref, geo_ref):
    geometry_kernel(corners_ref, conn_ref, seg_ref, slot_ref, geo_ref)
    place_kernel(copies, near, dest_ref, nodes_ref, out_ref, pick_ref)


def split_two(x):
    high = x.astype(jnp.bfloat16).astype(jnp.float32)
    return high, x - high


def split_three(x):
    high, rest = split_two(x)
    mid, low = split_two(rest)
    return high, mid, low


def ready_kernel(codes_ref, geo_ref, todo_ref, count_ref, left_ref, normal_ref):
    steps = left_ref.shape[0]
    each = codes_ref.shape[0] // steps
    row = lax.broadcasted_iota(jnp.int32, (8, BLK), 0)
    ends = [jnp.full((8, BLK), -1.0, jnp.float32), jnp.zeros((8, BLK), jnp.float32)]

    def two_blocks(b, count):
        stack = []
        for half in range(2):
            tile = geo_ref[pl.ds(pl.multiple_of(b * 16 + half * 8, 8), 8), :]
            square = jnp.sum(jnp.where(row < 3, tile * tile, 0.0), axis=0, keepdims=True) * -0.25
            high, mid, low = split_three(jnp.where(row == 7, square, tile))
            stack += [high, high, high, mid, mid, low] + ends
            high, low = split_two(tile[3:6])
            normal = jnp.concatenate([high, low, jnp.zeros((2, BLK), jnp.float32)], axis=0)
            normal_ref[b * 2 + half] = normal.astype(jnp.bfloat16)
        left_ref[b] = jnp.concatenate(stack, axis=0).astype(jnp.bfloat16).T
        for k in range(each):
            code = codes_ref[b * each + k]
            todo_ref[count] = code
            count = count + jnp.where(code >= 0, 1, 0)
        return count

    count = lax.fori_loop(0, steps, two_blocks, jnp.int32(0))
    for k in range(2 * TOGETHER):
        todo_ref[count + k] = NOBODY
    count_ref[0] = count


def force_kernel(todo_ref, count_ref, left_ref, normal_ref, nodes_ref, out_ref, total, press):
    near, _, slots, _ = out_ref.shape
    total[...] = jnp.zeros_like(total)
    row = lax.broadcasted_iota(jnp.int32, (8, BLK), 0)
    is_close = (row >= 3) & (row < 7)
    is_far = (row < 3) | (row == 7)
    zero = jnp.zeros((8, BLK), jnp.float32)
    nothing = jnp.zeros((64, 2 * BLK), jnp.bfloat16)

    def begin(k):
        for n in range(TOGETHER):
            code = todo_ref[k * TOGETHER + n]
            slot = code & 511
            block = code >> 9
            source = jnp.minimum(lax.div(slot, slots), near - 1)
            start = source * (6 * slots) + lax.rem(slot, slots)
            tile = nodes_ref[pl.ds(start, 6, stride=slots), :]
            square = jnp.sum(tile[0:3] * tile[0:3], axis=0, keepdims=True)
            high, mid, low = split_three(
                jnp.concatenate([tile, jnp.ones((2, BLK), jnp.float32)], axis=0)
            )
            order = [high, mid, low, high, mid, high]
            close = [jnp.where(is_close, part, 0.0) for part in order] + [zero, zero]
            high, mid, low = split_three(square)
            last = jnp.where(row == 0, high, jnp.where(row == 1, mid, jnp.where(row == 2, low, 0.0)))
            far = [jnp.where(is_far, part, 0.0) for part in order] + [last, zero]
            right = jnp.concatenate(
                [
                    jnp.concatenate(close, axis=0).astype(jnp.bfloat16),
                    jnp.concatenate(far, axis=0).astype(jnp.bfloat16),
                ],
                axis=1,
            )
            first = (block & 1) == 0
            right = jnp.concatenate(
                [jnp.where(first, right, nothing), jnp.where(first, nothing, right)], axis=0
            )
            both = jnp.dot(left_ref[block >> 1], right, preferred_element_type=jnp.float32)
            pressure = jnp.exp2(both[:, BLK:]) * jnp.maximum(both[:, :BLK], 0.0)
            high = pressure.astype(jnp.bfloat16)
            press[n, 0:BLK] = high
            press[n, BLK:] = (pressure - high.astype(jnp.float32)).astype(jnp.bfloat16)

    def finish(k):
        for n in range(TOGETHER):
            code = todo_ref[k * TOGETHER + n]
            normal = normal_ref[code >> 9]
            normal = jnp.concatenate([normal, normal], axis=1)
            force = jnp.dot(normal, press[n], preferred_element_type=jnp.float32)
            at = pl.ds(pl.multiple_of((code & 511) * 8, 8), 8)
            total[at, :] = total[at, :] + (force + pltpu.roll(force, 5, 0))

    def step(k, _):
        finish(k)
        begin(k + 1)
        return 0

    steps = lax.div(count_ref[0] + (TOGETHER - 1), TOGETHER)
    begin(0)
    lax.fori_loop(0, steps, step, 0)
    for source in range(near):
        for comp in range(3):
            for half in range(slots // 8):
                out_ref[source, comp, half * 8 : half * 8 + 8, :] = total[
                    pl.ds((source * slots + half * 8) * 8 + comp, 8, stride=8), :
                ]


def pick_kernel(pick_ref, back_ref, out_ref):
    for comp in range(3):
        rows = back_ref[:, comp].reshape(pick_ref.shape[1], BLK)
        out_ref[comp] = -STIFFNESS * exact_dot(pick_ref[...], rows)


def f32(*shape):
    return jax.ShapeDtypeStruct(shape, jnp.float32)


def contact(node_state, node_dest, seg_nodes, seg_conn, pair_seg, pair_slot):
    groups = lax.axis_size("grp")
    copies = lax.axis_size("zh")
    near = lax.axis_size(NEAR)
    blocks = node_state.shape[0]
    seg_blocks = seg_conn.shape[1] // BLK
    per_group = pair_seg.shape[2]
    slots = copies * 2
    owners = groups * copies
    total_blocks = owners * seg_blocks

    outgoing, pick, geometry = pl.pallas_call(
        functools.partial(start_kernel, copies, near),
        out_shape=(
            f32(near, 6, slots, BLK),
            jax.ShapeDtypeStruct((blocks, near * slots), jnp.bfloat16),
            f32(seg_blocks, 8, BLK),
        ),
        in_specs=[VMEM] * 6,
        out_specs=[VMEM] * 3,
    )(
        node_dest.reshape(1, blocks),
        jnp.transpose(node_state, (1, 0, 2)),
        seg_nodes,
        seg_conn,
        pair_seg,
        pair_slot,
    )
    received = lax.all_to_all(
        outgoing.reshape(near, 6 * slots, BLK), NEAR, split_axis=0, concat_axis=0, tiled=True
    )
    geometry = lax.all_gather(geometry.reshape(seg_blocks * 8, BLK), "zh", axis=0, tiled=True)
    geometry = lax.all_gather(geometry, "grp", axis=0, tiled=True)

    tables = geometry.reshape(owners, seg_blocks, 8, BLK)[:, :, 7, :per_group].astype(jnp.int32)
    row = lax.axis_index("grp")
    slot = lax.dynamic_index_in_dim(tables, row, axis=1, keepdims=False)
    seg = lax.dynamic_index_in_dim(tables, row + groups, axis=1, keepdims=False)
    owner = jnp.arange(owners, dtype=jnp.int32)[:, None]
    source = slot // 2
    place = (owner % copies) * 2 + slot % 2
    block = owner * seg_blocks + seg
    codes = (source % near) * slots + place + block * 512
    codes = jnp.where(source // near == lax.axis_index("zh"), codes, -1).reshape(-1)

    todo, count, left, normal = pl.pallas_call(
        ready_kernel,
        out_shape=(
            jax.ShapeDtypeStruct((codes.shape[0] + 2 * TOGETHER,), jnp.int32),
            jax.ShapeDtypeStruct((1,), jnp.int32),
            jax.ShapeDtypeStruct((total_blocks // 2, BLK, BLK), jnp.bfloat16),
            jax.ShapeDtypeStruct((total_blocks, 8, BLK), jnp.bfloat16),
        ),
        in_specs=[SMEM, VMEM],
        out_specs=[SMEM, SMEM, VMEM, VMEM],
        compiler_params=room(14),
    )(codes, geometry.reshape(total_blocks * 8, BLK))
    forces = pl.pallas_call(
        force_kernel,
        out_shape=f32(near, 3, slots, BLK),
        in_specs=[SMEM, SMEM, VMEM, VMEM, VMEM],
        out_specs=VMEM,
        scratch_shapes=[
            pltpu.VMEM(((near * slots + 1) * 8, BLK), jnp.float32),
            pltpu.VMEM((TOGETHER, 2 * BLK, BLK), jnp.bfloat16),
        ],
        compiler_params=room(20),
    )(todo, count, left, normal, received.reshape(near * 6 * slots, BLK))
    back = lax.all_to_all(
        forces.reshape(near, 3 * slots, BLK), NEAR, split_axis=0, concat_axis=0, tiled=True
    )
    out = pl.pallas_call(
        pick_kernel,
        out_shape=f32(3, blocks, BLK),
        in_specs=[VMEM] * 2,
        out_specs=VMEM,
        compiler_params=room(4),
    )(pick, back.reshape(near, 3, slots, BLK))
    return jnp.transpose(out, (1, 0, 2))


def solution(mesh):
    groups = mesh.shape["grp"]
    split = Mesh(mesh.devices.reshape(groups, COPIES, 16 // COPIES, 4, 2), GRP_DOM)
    placed = (
        P(GRP_DOM, None, None),
        P(GRP_DOM),
        P(None, GRP_DOM),
        P(None, GRP_DOM),
        P(GRP_DOM, None, None),
        P(GRP_DOM, None, None),
    )
    return jax.shard_map(contact, mesh=split, in_specs=placed, out_specs=P(GRP_DOM, None, None), check_vma=False)
```

```python
import functools
import math

import jax
import jax.numpy as jnp
from jax import lax
from jax.experimental import pallas as pl
from jax.experimental.pallas import tpu as pltpu
from jax.sharding import Mesh
from jax.sharding import PartitionSpec as P


BLK = 128
COPIES = 4
TIME_STEP = 0.5
STIFFNESS = 0.5
RADIUS_SQ = 0.5
SCALE = math.sqrt(math.log2(math.e) / RADIUS_SQ)
GRP_DOM = ("grp", "zh", "zl", "y", "core")
NEAR = ("zl", "y", "core")
VMEM = pl.BlockSpec(memory_space=pltpu.VMEM)
SMEM = pl.BlockSpec(memory_space=pltpu.SMEM)
TOGETHER = 8
NOBODY = 256


def room(mib):
    return pltpu.CompilerParams(vmem_limit_bytes=mib << 20)


def lane_pick(row, index):
    return jnp.take_along_axis(row, index, axis=1, mode="promise_in_bounds")


def geometry_kernel(nodes_ref, conn_ref, seg_ref, slot_ref, out_ref):
    blocks = conn_ref.shape[1] // BLK
    parts = nodes_ref.shape[1] // BLK
    index = [
        jnp.concatenate([conn_ref[k : k + 1, b * BLK : (b + 1) * BLK] for b in range(blocks)], axis=0)
        for k in range(3)
    ]
    lanes = [i & (BLK - 1) for i in index]
    part = [i >> 7 for i in index]
    corner = [[None] * 6 for _ in range(3)]
    for comp in range(6):
        for p in range(parts):
            row = jnp.broadcast_to(nodes_ref[comp : comp + 1, p * BLK : (p + 1) * BLK], (blocks, BLK))
            for k in range(3):
                got = lane_pick(row, lanes[k])
                corner[k][comp] = got if p == 0 else jnp.where(part[k] == p, got, corner[k][comp])
    a, b, c = corner
    e = [b[i] - a[i] for i in range(3)]
    f = [c[i] - a[i] for i in range(3)]
    n = [
        0.5 * (e[1] * f[2] - e[2] * f[1]),
        0.5 * (e[2] * f[0] - e[0] * f[2]),
        0.5 * (e[0] * f[1] - e[1] * f[0]),
    ]
    m = [(a[i] + b[i] + c[i]) / 3.0 for i in range(3)]
    u = [(a[i] + b[i] + c[i]) / 3.0 for i in range(3, 6)]
    s = sum(n[i] * (m[i] + TIME_STEP * u[i]) for i in range(3))
    rows = [m[i] * (2.0 * SCALE) for i in range(3)] + [-v for v in n] + [s]
    groups, each = slot_ref.shape[1:]
    tables = jnp.concatenate([slot_ref[0], seg_ref[0]], axis=0).astype(jnp.float32)
    tables = jnp.concatenate([tables, jnp.zeros((2 * groups, BLK - each), jnp.float32)], axis=1)
    for copy in range(out_ref.shape[0]):
        for i, row in enumerate(rows + [tables]):
            out_ref[copy, :, i, :] = row


def three_parts(x):
    high = x.astype(jnp.bfloat16)
    rest = x - high.astype(jnp.float32)
    mid = rest.astype(jnp.bfloat16)
    low = (rest - mid.astype(jnp.float32)).astype(jnp.bfloat16)
    return high, mid, low


def exact_dot(onehot, x):
    return sum(jnp.dot(onehot, part, preferred_element_type=jnp.float32) for part in three_parts(x))


def place_kernel(copies, near, dest_ref, nodes_ref, out_ref, pick_ref):
    blocks = dest_ref.shape[1]
    slots = near * copies * 2
    across = jnp.broadcast_to(dest_ref[...].astype(jnp.float32), (blocks, blocks))
    down = across.T
    i = lax.broadcasted_iota(jnp.int32, (blocks, blocks), 0)
    j = lax.broadcasted_iota(jnp.int32, (blocks, blocks), 1)
    same = across == down

    def slot_of(dest, rank):
        dest = dest.astype(jnp.int32)
        return ((dest & (near - 1)) * copies + lax.div(dest, near)) * 2 + rank.astype(jnp.int32)

    rank_row = jnp.sum(jnp.where(same & (i < j), 1.0, 0.0), axis=0, keepdims=True)
    slot_row = slot_of(dest_ref[...], rank_row)
    onehot = (lax.broadcasted_iota(jnp.int32, (slots, blocks), 0) == slot_row).astype(jnp.float32).astype(jnp.bfloat16)
    rank_col = jnp.sum(jnp.where(same & (j < i), 1.0, 0.0), axis=1, keepdims=True)
    slot_col = slot_of(down[:, 0:1], rank_col)
    pick_ref[...] = (
        (lax.broadcasted_iota(jnp.int32, (blocks, slots), 1) == slot_col).astype(jnp.float32).astype(jnp.bfloat16)
    )
    for comp in range(6):
        x = nodes_ref[comp % 3]
        row = x * SCALE if comp < 3 else x + TIME_STEP * nodes_ref[comp]
        out_ref[:, comp] = exact_dot(onehot, row).reshape(near, copies * 2, BLK)


def split_two(x):
    high = x.astype(jnp.bfloat16).astype(jnp.float32)
    return high, x - high


def split_three(x):
    high, rest = split_two(x)
    mid, low = split_two(rest)
    return high, mid, low


def ready_kernel(codes_ref, geo_ref, todo_ref, count_ref, left_ref):
    steps = left_ref.shape[0]
    each = codes_ref.shape[0] // steps
    row = lax.broadcasted_iota(jnp.int32, (8, BLK), 0)
    ends = [jnp.full((8, BLK), -1.0, jnp.float32), jnp.zeros((8, BLK), jnp.float32)]

    def two_blocks(b, count):
        stack = []
        for half in range(2):
            tile = geo_ref[pl.ds(pl.multiple_of(b * 16 + half * 8, 8), 8), :]
            square = jnp.sum(jnp.where(row < 3, tile * tile, 0.0), axis=0, keepdims=True) * -0.25
            high, mid, low = split_three(jnp.where(row == 7, square, tile))
            stack += [high, high, high, mid, mid, low] + ends
        left_ref[b] = jnp.concatenate(stack, axis=0).astype(jnp.bfloat16).T
        for k in range(each):
            code = codes_ref[b * each + k]
            todo_ref[count] = code
            count = count + jnp.where(code >= 0, 1, 0)
        return count

    count = lax.fori_loop(0, steps, two_blocks, jnp.int32(0), unroll=4)
    for k in range(2 * TOGETHER):
        todo_ref[count + k] = NOBODY
    count_ref[0] = count


def force_kernel(todo_ref, count_ref, left_ref, geo_ref, nodes_ref, out_ref, total, press):
    near, _, slots, _ = out_ref.shape
    total[...] = jnp.zeros_like(total)
    row = lax.broadcasted_iota(jnp.int32, (8, BLK), 0)
    is_close = (row >= 3) & (row < 7)
    is_far = (row < 3) | (row == 7)
    zero = jnp.zeros((8, BLK), jnp.float32)
    nothing = jnp.zeros((64, 2 * BLK), jnp.bfloat16)

    def begin(k):
        for n in range(TOGETHER):
            code = todo_ref[k * TOGETHER + n]
            slot = code & 511
            block = code >> 9
            source = jnp.minimum(lax.div(slot, slots), near - 1)
            start = source * (6 * slots) + lax.rem(slot, slots)
            tile = nodes_ref[pl.ds(start, 6, stride=slots), :]
            square = jnp.sum(tile[0:3] * tile[0:3], axis=0, keepdims=True)
            high, mid, low = split_three(
                jnp.concatenate([tile, jnp.ones((2, BLK), jnp.float32)], axis=0)
            )
            order = [high, mid, low, high, mid, high]
            close = [jnp.where(is_close, part, 0.0) for part in order] + [zero, zero]
            high, mid, low = split_three(square)
            last = jnp.where(row == 0, high, jnp.where(row == 1, mid, jnp.where(row == 2, low, 0.0)))
            far = [jnp.where(is_far, part, 0.0) for part in order] + [last, zero]
            right = jnp.concatenate(
                [
                    jnp.concatenate(close, axis=0).astype(jnp.bfloat16),
                    jnp.concatenate(far, axis=0).astype(jnp.bfloat16),
                ],
                axis=1,
            )
            first = (block & 1) == 0
            right = jnp.concatenate(
                [jnp.where(first, right, nothing), jnp.where(first, nothing, right)], axis=0
            )
            both = jnp.dot(left_ref[block >> 1], right, preferred_element_type=jnp.float32)
            pressure = jnp.exp2(both[:, BLK:]) * jnp.maximum(both[:, :BLK], 0.0)
            high = pressure.astype(jnp.bfloat16)
            press[n, 0:BLK] = high
            press[n, BLK:] = (pressure - high.astype(jnp.float32)).astype(jnp.bfloat16)

    def finish(k):
        for n in range(TOGETHER):
            code = todo_ref[k * TOGETHER + n]
            tile = geo_ref[pl.ds(pl.multiple_of((code >> 9) * 8, 8), 8), :]
            normal = jnp.concatenate(split_two(tile), axis=0).astype(jnp.bfloat16)
            normal = jnp.concatenate([normal, normal], axis=1)
            force = jnp.dot(normal, press[n], preferred_element_type=jnp.float32)
            at = pl.ds(pl.multiple_of((code & 511) * 8, 8), 8)
            total[at, :] = total[at, :] + (force[0:8] + force[8:16])

    def step(k, _):
        finish(k)
        begin(k + 1)
        return 0

    steps = lax.div(count_ref[0] + (TOGETHER - 1), TOGETHER)
    begin(0)
    lax.fori_loop(0, steps, step, 0)
    for source in range(near):
        for comp in range(3):
            for half in range(slots // 8):
                out_ref[source, comp, half * 8 : half * 8 + 8, :] = total[
                    pl.ds((source * slots + half * 8) * 8 + 3 + comp, 8, stride=8), :
                ]


def pick_kernel(pick_ref, back_ref, out_ref):
    for comp in range(3):
        rows = back_ref[:, comp].reshape(pick_ref.shape[1], BLK)
        out_ref[comp] = -STIFFNESS * exact_dot(pick_ref[...], rows)


def f32(*shape):
    return jax.ShapeDtypeStruct(shape, jnp.float32)


def contact(node_state, node_dest, seg_nodes, seg_conn, pair_seg, pair_slot):
    groups = lax.axis_size("grp")
    copies = lax.axis_size("zh")
    near = lax.axis_size(NEAR)
    blocks = node_state.shape[0]
    seg_blocks = seg_conn.shape[1] // BLK
    per_group = pair_seg.shape[2]
    slots = copies * 2
    owners = groups * copies
    total_blocks = owners * seg_blocks

    geometry = pl.pallas_call(
        geometry_kernel,
        out_shape=f32(1, seg_blocks, 8, BLK),
        in_specs=[VMEM] * 4,
        out_specs=VMEM,
    )(seg_nodes, seg_conn, pair_seg, pair_slot)
    outgoing, pick = pl.pallas_call(
        functools.partial(place_kernel, copies, near),
        out_shape=(f32(near, 6, slots, BLK), jax.ShapeDtypeStruct((blocks, near * slots), jnp.bfloat16)),
        in_specs=[VMEM] * 2,
        out_specs=[VMEM] * 2,
    )(node_dest.reshape(1, blocks), jnp.transpose(node_state, (1, 0, 2)))
    received = lax.all_to_all(
        outgoing.reshape(near, 6 * slots, BLK), NEAR, split_axis=0, concat_axis=0, tiled=True
    )
    geometry = geometry.reshape(seg_blocks * 8, BLK)
    offset = jnp.zeros((1,), jnp.int32)
    shift = 1
    while shift < copies:
        moved = lax.ppermute(geometry, "zh", [(i, i ^ shift) for i in range(copies)])
        geometry = jnp.concatenate([geometry, moved], axis=0)
        offset = jnp.concatenate([offset, offset ^ shift])
        shift *= 2
    geometry = lax.all_gather(geometry, "grp", axis=0, tiled=True)

    tables = geometry.reshape(owners, seg_blocks, 8, BLK)[:, :, 7, :per_group].astype(jnp.int32)
    row = lax.axis_index("grp")
    slot = lax.dynamic_index_in_dim(tables, row, axis=1, keepdims=False)
    seg = lax.dynamic_index_in_dim(tables, row + groups, axis=1, keepdims=False)
    owner = jnp.arange(owners, dtype=jnp.int32)[:, None]
    source = slot // 2
    place = (lax.axis_index("zh") ^ jnp.tile(offset, groups)[:, None]) * 2 + slot % 2
    block = owner * seg_blocks + seg
    codes = (source % near) * slots + place + block * 512
    codes = jnp.where(source // near == lax.axis_index("zh"), codes, -1).reshape(-1)

    todo, count, left = pl.pallas_call(
        ready_kernel,
        out_shape=(
            jax.ShapeDtypeStruct((codes.shape[0] + 2 * TOGETHER,), jnp.int32),
            jax.ShapeDtypeStruct((1,), jnp.int32),
            jax.ShapeDtypeStruct((total_blocks // 2, BLK, BLK), jnp.bfloat16),
        ),
        in_specs=[SMEM, VMEM],
        out_specs=[SMEM, SMEM, VMEM],
        compiler_params=room(14),
    )(codes, geometry)
    forces = pl.pallas_call(
        force_kernel,
        out_shape=f32(near, 3, slots, BLK),
        in_specs=[SMEM, SMEM, VMEM, VMEM, VMEM],
        out_specs=VMEM,
        scratch_shapes=[
            pltpu.VMEM(((near * slots + 1) * 8, BLK), jnp.float32),
            pltpu.VMEM((TOGETHER, 2 * BLK, BLK), jnp.bfloat16),
        ],
        compiler_params=room(20),
    )(todo, count, left, geometry, received.reshape(near * 6 * slots, BLK))
    back = lax.all_to_all(
        forces.reshape(near, 3 * slots, BLK), NEAR, split_axis=0, concat_axis=0, tiled=True
    )
    out = pl.pallas_call(
        pick_kernel,
        out_shape=f32(3, blocks, BLK),
        in_specs=[VMEM] * 2,
        out_specs=VMEM,
        compiler_params=room(4),
    )(pick, back.reshape(near, 3, slots, BLK))
    return jnp.transpose(out, (1, 0, 2))


def solution(mesh):
    groups = mesh.shape["grp"]
    split = Mesh(mesh.devices.reshape(groups, COPIES, 16 // COPIES, 4, 2), GRP_DOM)
    placed = (
        P(GRP_DOM, None, None),
        P(GRP_DOM),
        P(None, GRP_DOM),
        P(None, GRP_DOM),
        P(GRP_DOM, None, None),
        P(GRP_DOM, None, None),
    )
    return jax.shard_map(contact, mesh=split, in_specs=placed, out_specs=P(GRP_DOM, None, None), check_vma=False)
```

```python
import functools
import math

import jax
import jax.numpy as jnp
from jax import lax
from jax.experimental import pallas as pl
from jax.experimental.pallas import tpu as pltpu
from jax.sharding import Mesh
from jax.sharding import PartitionSpec as P


BLK = 128
COPIES = 4
TIME_STEP = 0.5
STIFFNESS = 0.5
RADIUS_SQ = 0.5
SCALE = math.sqrt(math.log2(math.e) / RADIUS_SQ)
GRP_DOM = ("grp", "zh", "zl", "y", "core")
NEAR = ("zl", "y", "core")
VMEM = pl.BlockSpec(memory_space=pltpu.VMEM)
SMEM = pl.BlockSpec(memory_space=pltpu.SMEM)
TOGETHER = 12
NOBODY = 256


def room(mib):
    return pltpu.CompilerParams(vmem_limit_bytes=mib << 20)


def lane_pick(row, index):
    return jnp.take_along_axis(row, index, axis=1, mode="promise_in_bounds")


def geometry_rows(nodes_ref, conn_ref, seg_ref, slot_ref, out_ref):
    blocks = conn_ref.shape[1] // BLK
    parts = nodes_ref.shape[1] // BLK
    index = [
        jnp.concatenate([conn_ref[k : k + 1, b * BLK : (b + 1) * BLK] for b in range(blocks)], axis=0)
        for k in range(3)
    ]
    lanes = [i & (BLK - 1) for i in index]
    part = [i >> 7 for i in index]
    corner = [[None] * 6 for _ in range(3)]
    for comp in range(6):
        for p in range(parts):
            row = jnp.broadcast_to(nodes_ref[comp : comp + 1, p * BLK : (p + 1) * BLK], (blocks, BLK))
            for k in range(3):
                got = lane_pick(row, lanes[k])
                corner[k][comp] = got if p == 0 else jnp.where(part[k] == p, got, corner[k][comp])
    a, b, c = corner
    e = [b[i] - a[i] for i in range(3)]
    f = [c[i] - a[i] for i in range(3)]
    n = [
        0.5 * (e[1] * f[2] - e[2] * f[1]),
        0.5 * (e[2] * f[0] - e[0] * f[2]),
        0.5 * (e[0] * f[1] - e[1] * f[0]),
    ]
    m = [(a[i] + b[i] + c[i]) / 3.0 for i in range(3)]
    u = [(a[i] + b[i] + c[i]) / 3.0 for i in range(3, 6)]
    s = sum(n[i] * (m[i] + TIME_STEP * u[i]) for i in range(3))
    rows = [m[i] * (2.0 * SCALE) for i in range(3)] + [-v for v in n] + [s]
    groups, each = slot_ref.shape[1:]
    tables = jnp.concatenate([slot_ref[0], seg_ref[0]], axis=0).astype(jnp.float32)
    tables = jnp.concatenate([tables, jnp.zeros((2 * groups, BLK - each), jnp.float32)], axis=1)
    for i, row in enumerate(rows + [tables]):
        out_ref[:, i, :] = row


def three_parts(x):
    high = x.astype(jnp.bfloat16)
    rest = x - high.astype(jnp.float32)
    mid = rest.astype(jnp.bfloat16)
    low = (rest - mid.astype(jnp.float32)).astype(jnp.bfloat16)
    return high, mid, low


def exact_dot(onehot, x):
    return sum(jnp.dot(onehot, part, preferred_element_type=jnp.float32) for part in three_parts(x))


def start_kernel(
    copies, near, dest_ref, nodes_ref, corners_ref, conn_ref, seg_ref, slot_ref, out_ref, pick_ref, geo_ref
):
    geometry_rows(corners_ref, conn_ref, seg_ref, slot_ref, geo_ref)
    blocks = dest_ref.shape[1]
    slots = near * copies * 2
    across = jnp.broadcast_to(dest_ref[...].astype(jnp.float32), (blocks, blocks))
    down = across.T
    i = lax.broadcasted_iota(jnp.int32, (blocks, blocks), 0)
    j = lax.broadcasted_iota(jnp.int32, (blocks, blocks), 1)
    same = across == down

    def slot_of(dest, rank):
        dest = dest.astype(jnp.int32)
        return ((dest & (near - 1)) * copies + lax.div(dest, near)) * 2 + rank.astype(jnp.int32)

    rank_row = jnp.sum(jnp.where(same & (i < j), 1.0, 0.0), axis=0, keepdims=True)
    slot_row = slot_of(dest_ref[...], rank_row)
    onehot = (lax.broadcasted_iota(jnp.int32, (slots, blocks), 0) == slot_row).astype(jnp.float32).astype(jnp.bfloat16)
    rank_col = jnp.sum(jnp.where(same & (j < i), 1.0, 0.0), axis=1, keepdims=True)
    slot_col = slot_of(down[:, 0:1], rank_col)
    pick_ref[...] = (
        (lax.broadcasted_iota(jnp.int32, (blocks, slots), 1) == slot_col).astype(jnp.float32).astype(jnp.bfloat16)
    )
    for comp in range(6):
        x = nodes_ref[comp % 3]
        row = x * SCALE if comp < 3 else x + TIME_STEP * nodes_ref[comp]
        out_ref[:, comp] = exact_dot(onehot, row).reshape(near, copies * 2, BLK)


def split_two(x):
    high = x.astype(jnp.bfloat16).astype(jnp.float32)
    return high, x - high


def split_three(x):
    high, rest = split_two(x)
    mid, low = split_two(rest)
    return high, mid, low


def force_kernel(codes_ref, geo_ref, nodes_ref, out_ref, total, press, todo_ref):
    near, _, slots, _ = out_ref.shape
    total[...] = jnp.zeros_like(total)
    row = lax.broadcasted_iota(jnp.int32, (8, BLK), 0)
    is_close = (row >= 3) & (row < 7)
    is_far = (row < 3) | (row == 7)
    zero = jnp.zeros((8, BLK), jnp.float32)
    minus = jnp.full((8, BLK), -1.0, jnp.float32)

    def geometry(code):
        return geo_ref[pl.ds(pl.multiple_of((code >> 9) * 8, 8), 8), :]

    def begin(k):
        for n in range(TOGETHER):
            code = todo_ref[k * TOGETHER + n]
            tile = geometry(code)
            square = jnp.sum(jnp.where(row < 3, tile * tile, 0.0), axis=0, keepdims=True) * -0.25
            high, mid, low = split_three(jnp.where(row == 7, square, tile))
            left = jnp.concatenate([high, high, high, mid, mid, low, minus, zero], axis=0)
            left = left.astype(jnp.bfloat16).T

            slot = code & 511
            source = jnp.minimum(lax.div(slot, slots), near - 1)
            start = source * (6 * slots) + lax.rem(slot, slots)
            tile = nodes_ref[pl.ds(start, 6, stride=slots), :]
            square = jnp.sum(tile[0:3] * tile[0:3], axis=0, keepdims=True)
            high, mid, low = split_three(
                jnp.concatenate([tile, jnp.ones((2, BLK), jnp.float32)], axis=0)
            )
            order = [high, mid, low, high, mid, high]
            close = [jnp.where(is_close, part, 0.0) for part in order] + [zero, zero]
            high, mid, low = split_three(square)
            last = jnp.where(row == 0, high, jnp.where(row == 1, mid, jnp.where(row == 2, low, 0.0)))
            far = [jnp.where(is_far, part, 0.0) for part in order] + [last, zero]
            right = jnp.concatenate(
                [
                    jnp.concatenate(close, axis=0).astype(jnp.bfloat16),
                    jnp.concatenate(far, axis=0).astype(jnp.bfloat16),
                ],
                axis=1,
            )
            both = jnp.dot(left, right, preferred_element_type=jnp.float32)
            pressure = jnp.exp2(both[:, BLK:]) * jnp.maximum(both[:, :BLK], 0.0)
            high = pressure.astype(jnp.bfloat16)
            press[n, 0:BLK] = high
            press[n, BLK:] = (pressure - high.astype(jnp.float32)).astype(jnp.bfloat16)

    def finish(k):
        for n in range(TOGETHER):
            code = todo_ref[k * TOGETHER + n]
            normal = jnp.concatenate(split_two(geometry(code)), axis=0).astype(jnp.bfloat16)
            normal = jnp.concatenate([normal, normal], axis=1)
            force = jnp.dot(normal, press[n], preferred_element_type=jnp.float32)
            at = pl.ds(pl.multiple_of((code & 511) * 8, 8), 8)
            total[at, :] = total[at, :] + (force[0:8] + force[8:16])

    def step(k, _):
        finish(k)
        begin(k + 1)
        return 0

    def keep(k, count):
        code = codes_ref[k]
        todo_ref[count] = code
        return count + 1 + (code >> 31)

    count = lax.fori_loop(0, codes_ref.shape[0], keep, jnp.int32(0), unroll=16)
    for k in range(2 * TOGETHER):
        todo_ref[count + k] = NOBODY
    steps = lax.div(count + (TOGETHER - 1), TOGETHER)
    begin(0)
    lax.fori_loop(0, steps, step, 0)
    for source in range(near):
        for comp in range(3):
            for half in range(slots // 8):
                out_ref[source, comp, half * 8 : half * 8 + 8, :] = total[
                    pl.ds((source * slots + half * 8) * 8 + 3 + comp, 8, stride=8), :
                ]


def pick_kernel(pick_ref, back_ref, out_ref):
    for comp in range(3):
        rows = back_ref[:, comp].reshape(pick_ref.shape[1], BLK)
        out_ref[comp] = -STIFFNESS * exact_dot(pick_ref[...], rows)


def f32(*shape):
    return jax.ShapeDtypeStruct(shape, jnp.float32)


def contact(node_state, node_dest, seg_nodes, seg_conn, pair_seg, pair_slot):
    groups = lax.axis_size("grp")
    copies = lax.axis_size("zh")
    near = lax.axis_size(NEAR)
    blocks = node_state.shape[0]
    seg_blocks = seg_conn.shape[1] // BLK
    per_group = pair_seg.shape[2]
    slots = copies * 2
    owners = groups * copies

    outgoing, pick, geometry = pl.pallas_call(
        functools.partial(start_kernel, copies, near),
        out_shape=(
            f32(near, 6, slots, BLK),
            jax.ShapeDtypeStruct((blocks, near * slots), jnp.bfloat16),
            f32(seg_blocks, 8, BLK),
        ),
        in_specs=[VMEM] * 6,
        out_specs=[VMEM] * 3,
    )(
        node_dest.reshape(1, blocks),
        jnp.transpose(node_state, (1, 0, 2)),
        seg_nodes,
        seg_conn,
        pair_seg,
        pair_slot,
    )
    geometry = geometry.reshape(seg_blocks * 8, BLK)
    pieces = [geometry]
    for other in range(1, copies):
        pieces.append(lax.ppermute(geometry, "zh", [(i, i ^ other) for i in range(copies)]))
    received = lax.all_to_all(
        outgoing.reshape(near, 6 * slots, BLK), NEAR, split_axis=0, concat_axis=0, tiled=True
    )
    geometry = lax.all_gather(jnp.concatenate(pieces, axis=0), "grp", axis=0, tiled=True)

    tables = geometry.reshape(owners, seg_blocks, 8, BLK)[:, :, 7, :per_group].astype(jnp.int32)
    row = lax.axis_index("grp")
    slot = lax.dynamic_index_in_dim(tables, row, axis=1, keepdims=False)
    seg = lax.dynamic_index_in_dim(tables, row + groups, axis=1, keepdims=False)
    owner = jnp.arange(owners, dtype=jnp.int32)[:, None]
    source = slot // 2
    place = (lax.axis_index("zh") ^ (owner % copies)) * 2 + slot % 2
    block = owner * seg_blocks + seg
    codes = (source % near) * slots + place + block * 512
    codes = jnp.where(source // near == lax.axis_index("zh"), codes, -1).reshape(-1)

    forces = pl.pallas_call(
        force_kernel,
        out_shape=f32(near, 3, slots, BLK),
        in_specs=[SMEM, VMEM, VMEM],
        out_specs=VMEM,
        scratch_shapes=[
            pltpu.VMEM(((near * slots + 1) * 8, BLK), jnp.float32),
            pltpu.VMEM((TOGETHER, 2 * BLK, BLK), jnp.bfloat16),
            pltpu.SMEM((codes.shape[0] + 2 * TOGETHER,), jnp.int32),
        ],
        compiler_params=room(20),
    )(codes, geometry, received.reshape(near * 6 * slots, BLK))
    back = lax.all_to_all(
        forces.reshape(near, 3 * slots, BLK), NEAR, split_axis=0, concat_axis=0, tiled=True
    )
    out = pl.pallas_call(
        pick_kernel,
        out_shape=f32(3, blocks, BLK),
        in_specs=[VMEM] * 2,
        out_specs=VMEM,
        compiler_params=room(4),
    )(pick, back.reshape(near, 3, slots, BLK))
    return jnp.transpose(out, (1, 0, 2))


def solution(mesh):
    groups = mesh.shape["grp"]
    split = Mesh(mesh.devices.reshape(groups, COPIES, 16 // COPIES, 4, 2), GRP_DOM)
    placed = (
        P(GRP_DOM, None, None),
        P(GRP_DOM),
        P(None, GRP_DOM),
        P(None, GRP_DOM),
        P(GRP_DOM, None, None),
        P(GRP_DOM, None, None),
    )
    return jax.shard_map(contact, mesh=split, in_specs=placed, out_specs=P(GRP_DOM, None, None), check_vma=False)
```

```python
import functools
import math

import jax
import jax.numpy as jnp
from jax import lax
from jax.experimental import pallas as pl
from jax.experimental.pallas import tpu as pltpu
from jax.sharding import Mesh
from jax.sharding import PartitionSpec as P


BLK = 128
COPIES = 4
TIME_STEP = 0.5
STIFFNESS = 0.5
RADIUS_SQ = 0.5
SCALE = math.sqrt(math.log2(math.e) / RADIUS_SQ)
GRP_DOM = ("grp", "zh", "zl", "y", "core")
NEAR = ("zl", "y", "core")
VMEM = pl.BlockSpec(memory_space=pltpu.VMEM)
SMEM = pl.BlockSpec(memory_space=pltpu.SMEM)
TOGETHER = 16
NOBODY = 256


def room(mib):
    return pltpu.CompilerParams(vmem_limit_bytes=mib << 20)


def lane_pick(row, index):
    return jnp.take_along_axis(row, index, axis=1, mode="promise_in_bounds")


def geometry_rows(nodes_ref, conn_ref, seg_ref, slot_ref, out_ref):
    blocks = conn_ref.shape[1] // BLK
    parts = nodes_ref.shape[1] // BLK
    index = [
        jnp.concatenate([conn_ref[k : k + 1, b * BLK : (b + 1) * BLK] for b in range(blocks)], axis=0)
        for k in range(3)
    ]
    lanes = [i & (BLK - 1) for i in index]
    part = [i >> 7 for i in index]
    corner = [[None] * 6 for _ in range(3)]
    for comp in range(6):
        for p in range(parts):
            row = jnp.broadcast_to(nodes_ref[comp : comp + 1, p * BLK : (p + 1) * BLK], (blocks, BLK))
            for k in range(3):
                got = lane_pick(row, lanes[k])
                corner[k][comp] = got if p == 0 else jnp.where(part[k] == p, got, corner[k][comp])
    a, b, c = corner
    e = [b[i] - a[i] for i in range(3)]
    f = [c[i] - a[i] for i in range(3)]
    n = [
        0.5 * (e[1] * f[2] - e[2] * f[1]),
        0.5 * (e[2] * f[0] - e[0] * f[2]),
        0.5 * (e[0] * f[1] - e[1] * f[0]),
    ]
    m = [(a[i] + b[i] + c[i]) / 3.0 for i in range(3)]
    u = [(a[i] + b[i] + c[i]) / 3.0 for i in range(3, 6)]
    s = sum(n[i] * (m[i] + TIME_STEP * u[i]) for i in range(3))
    rows = [m[i] * (2.0 * SCALE) for i in range(3)] + [-v for v in n] + [s]
    groups, each = slot_ref.shape[1:]
    tables = jnp.concatenate([slot_ref[0], seg_ref[0]], axis=0).astype(jnp.float32)
    tables = jnp.concatenate([tables, jnp.zeros((2 * groups, BLK - each), jnp.float32)], axis=1)
    for i, row in enumerate(rows + [tables]):
        out_ref[:, i, :] = row


def three_parts(x):
    high = x.astype(jnp.bfloat16)
    rest = x - high.astype(jnp.float32)
    mid = rest.astype(jnp.bfloat16)
    low = (rest - mid.astype(jnp.float32)).astype(jnp.bfloat16)
    return high, mid, low


def exact_dot(onehot, x):
    return sum(jnp.dot(onehot, part, preferred_element_type=jnp.float32) for part in three_parts(x))


def start_kernel(
    copies, near, dest_ref, nodes_ref, corners_ref, conn_ref, seg_ref, slot_ref, out_ref, pick_ref, geo_ref
):
    geometry_rows(corners_ref, conn_ref, seg_ref, slot_ref, geo_ref)
    blocks = dest_ref.shape[1]
    slots = near * copies * 2
    across = jnp.broadcast_to(dest_ref[...].astype(jnp.float32), (blocks, blocks))
    down = across.T
    i = lax.broadcasted_iota(jnp.int32, (blocks, blocks), 0)
    j = lax.broadcasted_iota(jnp.int32, (blocks, blocks), 1)
    same = across == down

    def slot_of(dest, rank):
        dest = dest.astype(jnp.int32)
        return ((dest & (near - 1)) * copies + lax.div(dest, near)) * 2 + rank.astype(jnp.int32)

    rank_row = jnp.sum(jnp.where(same & (i < j), 1.0, 0.0), axis=0, keepdims=True)
    slot_row = slot_of(dest_ref[...], rank_row)
    onehot = (lax.broadcasted_iota(jnp.int32, (slots, blocks), 0) == slot_row).astype(jnp.float32).astype(jnp.bfloat16)
    rank_col = jnp.sum(jnp.where(same & (j < i), 1.0, 0.0), axis=1, keepdims=True)
    slot_col = slot_of(down[:, 0:1], rank_col)
    pick_ref[...] = (
        (lax.broadcasted_iota(jnp.int32, (blocks, slots), 1) == slot_col).astype(jnp.float32).astype(jnp.bfloat16)
    )
    for comp in range(6):
        x = nodes_ref[comp % 3]
        row = x * SCALE if comp < 3 else x + TIME_STEP * nodes_ref[comp]
        out_ref[:, comp] = exact_dot(onehot, row).reshape(near, copies * 2, BLK)


def split_two(x):
    high = x.astype(jnp.bfloat16).astype(jnp.float32)
    return high, x - high


def split_three(x):
    high, rest = split_two(x)
    mid, low = split_two(rest)
    return high, mid, low


def force_kernel(codes_ref, geo_ref, nodes_ref, out_ref, total, press, todo_ref):
    near, _, slots, _ = out_ref.shape
    total[...] = jnp.zeros_like(total)
    row = lax.broadcasted_iota(jnp.int32, (8, BLK), 0)
    is_close = (row >= 3) & (row < 7)
    is_far = (row < 3) | (row == 7)
    zero = jnp.zeros((8, BLK), jnp.float32)
    minus = jnp.full((8, BLK), -1.0, jnp.float32)

    def geometry(code):
        return geo_ref[pl.ds(pl.multiple_of((code >> 9) * 8, 8), 8), :]

    def begin(k):
        for n in range(TOGETHER):
            code = todo_ref[k * TOGETHER + n]
            tile = geometry(code)
            square = jnp.sum(jnp.where(row < 3, tile * tile, 0.0), axis=0, keepdims=True) * -0.25
            high, mid, low = split_three(jnp.where(row == 7, square, tile))
            left = jnp.concatenate([high, high, high, mid, mid, low, minus, zero], axis=0)
            left = left.astype(jnp.bfloat16).T

            slot = code & 511
            source = jnp.minimum(lax.div(slot, slots), near - 1)
            start = source * (6 * slots) + lax.rem(slot, slots)
            tile = nodes_ref[pl.ds(start, 6, stride=slots), :]
            square = jnp.sum(tile[0:3] * tile[0:3], axis=0, keepdims=True)
            high, mid, low = split_three(
                jnp.concatenate([tile, jnp.ones((2, BLK), jnp.float32)], axis=0)
            )
            order = [high, mid, low, high, mid, high]
            close = [jnp.where(is_close, part, 0.0) for part in order] + [zero, zero]
            high, mid, low = split_three(square)
            last = jnp.where(row == 0, high, jnp.where(row == 1, mid, jnp.where(row == 2, low, 0.0)))
            far = [jnp.where(is_far, part, 0.0) for part in order] + [last, zero]
            right = jnp.concatenate(
                [
                    jnp.concatenate(close, axis=0).astype(jnp.bfloat16),
                    jnp.concatenate(far, axis=0).astype(jnp.bfloat16),
                ],
                axis=1,
            )
            both = jnp.dot(left, right, preferred_element_type=jnp.float32)
            pressure = jnp.exp2(both[:, BLK:]) * jnp.maximum(both[:, :BLK], 0.0)
            high = pressure.astype(jnp.bfloat16)
            press[n, 0:BLK] = high
            press[n, BLK:] = (pressure - high.astype(jnp.float32)).astype(jnp.bfloat16)

    def finish(k):
        for n in range(TOGETHER):
            code = todo_ref[k * TOGETHER + n]
            normal = jnp.concatenate(split_two(geometry(code)), axis=0).astype(jnp.bfloat16)
            normal = jnp.concatenate([normal, normal], axis=1)
            force = jnp.dot(normal, press[n], preferred_element_type=jnp.float32)
            at = pl.ds(pl.multiple_of((code & 511) * 8, 8), 8)
            total[at, :] = total[at, :] + (force[0:8] + force[8:16])

    def step(k, _):
        finish(k)
        begin(k + 1)
        return 0

    def keep(k, count):
        code = codes_ref[k]
        todo_ref[count] = code
        return count + 1 + (code >> 31)

    count = lax.fori_loop(0, codes_ref.shape[0], keep, jnp.int32(0), unroll=64)
    for k in range(2 * TOGETHER):
        todo_ref[count + k] = NOBODY
    last = jnp.maximum(lax.div(count + (TOGETHER - 1), TOGETHER) - 1, 0)
    begin(0)
    lax.fori_loop(0, last, step, 0)
    finish(last)
    for source in range(near):
        for comp in range(3):
            for half in range(slots // 8):
                out_ref[source, comp, half * 8 : half * 8 + 8, :] = total[
                    pl.ds((source * slots + half * 8) * 8 + 3 + comp, 8, stride=8), :
                ]


def pick_kernel(pick_ref, back_ref, out_ref):
    for comp in range(3):
        rows = back_ref[:, comp].reshape(pick_ref.shape[1], BLK)
        out_ref[comp] = -STIFFNESS * exact_dot(pick_ref[...], rows)


def f32(*shape):
    return jax.ShapeDtypeStruct(shape, jnp.float32)


def contact(node_state, node_dest, seg_nodes, seg_conn, pair_seg, pair_slot):
    groups = lax.axis_size("grp")
    copies = lax.axis_size("zh")
    near = lax.axis_size(NEAR)
    blocks = node_state.shape[0]
    seg_blocks = seg_conn.shape[1] // BLK
    per_group = pair_seg.shape[2]
    slots = copies * 2
    owners = groups * copies

    outgoing, pick, geometry = pl.pallas_call(
        functools.partial(start_kernel, copies, near),
        out_shape=(
            f32(near, 6, slots, BLK),
            jax.ShapeDtypeStruct((blocks, near * slots), jnp.bfloat16),
            f32(seg_blocks, 8, BLK),
        ),
        in_specs=[VMEM] * 6,
        out_specs=[VMEM] * 3,
    )(
        node_dest.reshape(1, blocks),
        jnp.transpose(node_state, (1, 0, 2)),
        seg_nodes,
        seg_conn,
        pair_seg,
        pair_slot,
    )
    geometry = geometry.reshape(seg_blocks * 8, BLK)
    pieces = [geometry]
    for other in range(1, copies):
        pieces.append(lax.ppermute(geometry, "zh", [(i, i ^ other) for i in range(copies)]))
    received = lax.all_to_all(
        outgoing.reshape(near, 6 * slots, BLK), NEAR, split_axis=0, concat_axis=0, tiled=True
    )
    geometry = lax.all_gather(jnp.concatenate(pieces, axis=0), "grp", axis=0, tiled=True)

    tables = geometry.reshape(owners, seg_blocks, 8, BLK)[:, :, 7, :per_group].astype(jnp.int32)
    row = lax.axis_index("grp")
    slot = lax.dynamic_index_in_dim(tables, row, axis=1, keepdims=False)
    seg = lax.dynamic_index_in_dim(tables, row + groups, axis=1, keepdims=False)
    owner = jnp.arange(owners, dtype=jnp.int32)[:, None]
    source = slot // 2
    place = (lax.axis_index("zh") ^ (owner % copies)) * 2 + slot % 2
    block = owner * seg_blocks + seg
    codes = (source % near) * slots + place + block * 512
    codes = jnp.where(source // near == lax.axis_index("zh"), codes, -1).reshape(-1)

    forces = pl.pallas_call(
        force_kernel,
        out_shape=f32(near, 3, slots, BLK),
        in_specs=[SMEM, VMEM, VMEM],
        out_specs=VMEM,
        scratch_shapes=[
            pltpu.VMEM(((near * slots + 1) * 8, BLK), jnp.float32),
            pltpu.VMEM((TOGETHER, 2 * BLK, BLK), jnp.bfloat16),
            pltpu.SMEM((codes.shape[0] + 2 * TOGETHER,), jnp.int32),
        ],
        compiler_params=room(20),
    )(codes, geometry, received.reshape(near * 6 * slots, BLK))
    back = lax.all_to_all(
        forces.reshape(near, 3 * slots, BLK), NEAR, split_axis=0, concat_axis=0, tiled=True
    )
    out = pl.pallas_call(
        pick_kernel,
        out_shape=f32(3, blocks, BLK),
        in_specs=[VMEM] * 2,
        out_specs=VMEM,
        compiler_params=room(4),
    )(pick, back.reshape(near, 3, slots, BLK))
    return jnp.transpose(out, (1, 0, 2))


def solution(mesh):
    groups = mesh.shape["grp"]
    split = Mesh(mesh.devices.reshape(groups, COPIES, 16 // COPIES, 4, 2), GRP_DOM)
    placed = (
        P(GRP_DOM, None, None),
        P(GRP_DOM),
        P(None, GRP_DOM),
        P(None, GRP_DOM),
        P(GRP_DOM, None, None),
        P(GRP_DOM, None, None),
    )
    return jax.shard_map(contact, mesh=split, in_specs=placed, out_specs=P(GRP_DOM, None, None), check_vma=False)
```

```python
import functools
import math

import jax
import jax.numpy as jnp
from jax import lax
from jax.experimental import pallas as pl
from jax.experimental.pallas import tpu as pltpu
from jax.sharding import Mesh
from jax.sharding import PartitionSpec as P


BLK = 128
COPIES = 4
TIME_STEP = 0.5
STIFFNESS = 0.5
RADIUS_SQ = 0.5
SCALE = math.sqrt(math.log2(math.e) / RADIUS_SQ)
GRP_DOM = ("grp", "zh", "zl", "y", "core")
NEAR = ("zl", "y", "core")
VMEM = pl.BlockSpec(memory_space=pltpu.VMEM)
SMEM = pl.BlockSpec(memory_space=pltpu.SMEM)
TOGETHER = 16
NOBODY = 256


def room(mib):
    return pltpu.CompilerParams(vmem_limit_bytes=mib << 20)


def lane_pick(row, index):
    return jnp.take_along_axis(row, index, axis=1, mode="promise_in_bounds")


def geometry_rows(nodes_ref, conn_ref, seg_ref, slot_ref, out_ref):
    blocks = conn_ref.shape[1] // BLK
    parts = nodes_ref.shape[1] // BLK
    index = [
        jnp.concatenate([conn_ref[k : k + 1, b * BLK : (b + 1) * BLK] for b in range(blocks)], axis=0)
        for k in range(3)
    ]
    lanes = [i & (BLK - 1) for i in index]
    part = [i >> 7 for i in index]
    corner = [[None] * 6 for _ in range(3)]
    for comp in range(6):
        for p in range(parts):
            row = jnp.broadcast_to(nodes_ref[comp : comp + 1, p * BLK : (p + 1) * BLK], (blocks, BLK))
            for k in range(3):
                got = lane_pick(row, lanes[k])
                corner[k][comp] = got if p == 0 else jnp.where(part[k] == p, got, corner[k][comp])
    a, b, c = corner
    e = [b[i] - a[i] for i in range(3)]
    f = [c[i] - a[i] for i in range(3)]
    n = [
        0.5 * (e[1] * f[2] - e[2] * f[1]),
        0.5 * (e[2] * f[0] - e[0] * f[2]),
        0.5 * (e[0] * f[1] - e[1] * f[0]),
    ]
    m = [(a[i] + b[i] + c[i]) / 3.0 for i in range(3)]
    u = [(a[i] + b[i] + c[i]) / 3.0 for i in range(3, 6)]
    s = sum(n[i] * (m[i] + TIME_STEP * u[i]) for i in range(3))
    rows = [m[i] * (2.0 * SCALE) for i in range(3)] + [-v for v in n] + [s]
    groups, each = slot_ref.shape[1:]
    tables = jnp.concatenate([slot_ref[0], seg_ref[0]], axis=0).astype(jnp.float32)
    tables = jnp.concatenate([tables, jnp.zeros((2 * groups, BLK - each), jnp.float32)], axis=1)
    for i, row in enumerate(rows + [tables]):
        out_ref[:, i, :] = row


def three_parts(x):
    high = x.astype(jnp.bfloat16)
    rest = x - high.astype(jnp.float32)
    mid = rest.astype(jnp.bfloat16)
    low = (rest - mid.astype(jnp.float32)).astype(jnp.bfloat16)
    return high, mid, low


def exact_dot(onehot, x):
    return sum(jnp.dot(onehot, part, preferred_element_type=jnp.float32) for part in three_parts(x))


def start_kernel(
    copies, near, dest_ref, nodes_ref, corners_ref, conn_ref, seg_ref, slot_ref, out_ref, pick_ref, geo_ref
):
    geometry_rows(corners_ref, conn_ref, seg_ref, slot_ref, geo_ref)
    blocks = dest_ref.shape[1]
    slots = near * copies * 2
    across = jnp.broadcast_to(dest_ref[...].astype(jnp.float32), (blocks, blocks))
    down = across.T
    i = lax.broadcasted_iota(jnp.int32, (blocks, blocks), 0)
    j = lax.broadcasted_iota(jnp.int32, (blocks, blocks), 1)
    same = across == down

    def slot_of(dest, rank):
        dest = dest.astype(jnp.int32)
        return ((dest & (near - 1)) * copies + lax.div(dest, near)) * 2 + rank.astype(jnp.int32)

    rank_row = jnp.sum(jnp.where(same & (i < j), 1.0, 0.0), axis=0, keepdims=True)
    slot_row = slot_of(dest_ref[...], rank_row)
    onehot = (lax.broadcasted_iota(jnp.int32, (slots, blocks), 0) == slot_row).astype(jnp.float32).astype(jnp.bfloat16)
    rank_col = jnp.sum(jnp.where(same & (j < i), 1.0, 0.0), axis=1, keepdims=True)
    slot_col = slot_of(down[:, 0:1], rank_col)
    pick_ref[...] = (
        (lax.broadcasted_iota(jnp.int32, (blocks, slots), 1) == slot_col).astype(jnp.float32).astype(jnp.bfloat16)
    )
    for comp in range(6):
        x = nodes_ref[comp % 3]
        row = x * SCALE if comp < 3 else x + TIME_STEP * nodes_ref[comp]
        out_ref[:, comp] = exact_dot(onehot, row).reshape(near, copies * 2, BLK)


def split_two(x):
    high = x.astype(jnp.bfloat16).astype(jnp.float32)
    return high, x - high


def split_three(x):
    high, rest = split_two(x)
    mid, low = split_two(rest)
    return high, mid, low


def list_kernel(codes_ref, todo_ref, count_ref):
    def keep(k, count):
        code = codes_ref[k]
        todo_ref[count] = code
        return count + 1 + (code >> 31)

    count = lax.fori_loop(0, codes_ref.shape[0], keep, jnp.int32(0), unroll=64)
    for k in range(2 * TOGETHER):
        todo_ref[count + k] = NOBODY
    count_ref[0] = count


def force_kernel(todo_ref, count_ref, geo_ref, nodes_ref, out_ref, total, press):
    near, _, slots, _ = out_ref.shape
    total[...] = jnp.zeros_like(total)
    row = lax.broadcasted_iota(jnp.int32, (8, BLK), 0)
    is_close = (row >= 3) & (row < 7)
    is_far = (row < 3) | (row == 7)
    zero = jnp.zeros((8, BLK), jnp.float32)
    minus = jnp.full((8, BLK), -1.0, jnp.float32)

    def geometry(code):
        return geo_ref[pl.ds(pl.multiple_of((code >> 9) * 8, 8), 8), :]

    def begin(k):
        for n in range(TOGETHER):
            code = todo_ref[k * TOGETHER + n]
            tile = geometry(code)
            square = jnp.sum(jnp.where(row < 3, tile * tile, 0.0), axis=0, keepdims=True) * -0.25
            high, mid, low = split_three(jnp.where(row == 7, square, tile))
            left = jnp.concatenate([high, high, high, mid, mid, low, minus, zero], axis=0)
            left = left.astype(jnp.bfloat16).T

            slot = code & 511
            source = jnp.minimum(lax.div(slot, slots), near - 1)
            start = source * (6 * slots) + lax.rem(slot, slots)
            tile = nodes_ref[pl.ds(start, 6, stride=slots), :]
            square = jnp.sum(tile[0:3] * tile[0:3], axis=0, keepdims=True)
            high, mid, low = split_three(
                jnp.concatenate([tile, jnp.ones((2, BLK), jnp.float32)], axis=0)
            )
            order = [high, mid, low, high, mid, high]
            close = [jnp.where(is_close, part, 0.0) for part in order] + [zero, zero]
            high, mid, low = split_three(square)
            last = jnp.where(row == 0, high, jnp.where(row == 1, mid, jnp.where(row == 2, low, 0.0)))
            far = [jnp.where(is_far, part, 0.0) for part in order] + [last, zero]
            right = jnp.concatenate(
                [
                    jnp.concatenate(close, axis=0).astype(jnp.bfloat16),
                    jnp.concatenate(far, axis=0).astype(jnp.bfloat16),
                ],
                axis=1,
            )
            both = jnp.dot(left, right, preferred_element_type=jnp.float32)
            pressure = jnp.exp2(both[:, BLK:]) * jnp.maximum(both[:, :BLK], 0.0)
            high = pressure.astype(jnp.bfloat16)
            press[n, 0:BLK] = high
            press[n, BLK:] = (pressure - high.astype(jnp.float32)).astype(jnp.bfloat16)

    def finish(k):
        for n in range(TOGETHER):
            code = todo_ref[k * TOGETHER + n]
            normal = jnp.concatenate(split_two(geometry(code)), axis=0).astype(jnp.bfloat16)
            normal = jnp.concatenate([normal, normal], axis=1)
            force = jnp.dot(normal, press[n], preferred_element_type=jnp.float32)
            at = pl.ds(pl.multiple_of((code & 511) * 8, 8), 8)
            total[at, :] = total[at, :] + (force[0:8] + force[8:16])

    def step(k, _):
        finish(k)
        begin(k + 1)
        return 0

    last = jnp.maximum(lax.div(count_ref[0] + (TOGETHER - 1), TOGETHER) - 1, 0)
    begin(0)
    lax.fori_loop(0, last, step, 0)
    finish(last)
    for source in range(near):
        for comp in range(3):
            for half in range(slots // 8):
                out_ref[source, comp, half * 8 : half * 8 + 8, :] = total[
                    pl.ds((source * slots + half * 8) * 8 + 3 + comp, 8, stride=8), :
                ]


def pick_kernel(pick_ref, back_ref, out_ref):
    for comp in range(3):
        rows = back_ref[:, comp].reshape(pick_ref.shape[1], BLK)
        out_ref[comp] = -STIFFNESS * exact_dot(pick_ref[...], rows)


def f32(*shape):
    return jax.ShapeDtypeStruct(shape, jnp.float32)


def contact(node_state, node_dest, seg_nodes, seg_conn, pair_seg, pair_slot):
    groups = lax.axis_size("grp")
    copies = lax.axis_size("zh")
    near = lax.axis_size(NEAR)
    blocks = node_state.shape[0]
    seg_blocks = seg_conn.shape[1] // BLK
    per_group = pair_seg.shape[2]
    slots = copies * 2
    owners = groups * copies

    outgoing, pick, geometry = pl.pallas_call(
        functools.partial(start_kernel, copies, near),
        out_shape=(
            f32(near, 6, slots, BLK),
            jax.ShapeDtypeStruct((blocks, near * slots), jnp.bfloat16),
            f32(seg_blocks, 8, BLK),
        ),
        in_specs=[VMEM] * 6,
        out_specs=[VMEM] * 3,
    )(
        node_dest.reshape(1, blocks),
        jnp.transpose(node_state, (1, 0, 2)),
        seg_nodes,
        seg_conn,
        pair_seg,
        pair_slot,
    )
    geometry = geometry.reshape(seg_blocks * 8, BLK)
    pieces = [geometry]
    for other in range(1, copies):
        pieces.append(lax.ppermute(geometry, "zh", [(i, i ^ other) for i in range(copies)]))
    received = lax.all_to_all(
        outgoing.reshape(near, 6 * slots, BLK), NEAR, split_axis=0, concat_axis=0, tiled=True
    )
    geometry = lax.all_gather(jnp.concatenate(pieces, axis=0), "grp", axis=0, tiled=True)

    tables = geometry.reshape(owners, seg_blocks, 8, BLK)[:, :, 7, :per_group].astype(jnp.int32)
    row = lax.axis_index("grp")
    slot = lax.dynamic_index_in_dim(tables, row, axis=1, keepdims=False)
    seg = lax.dynamic_index_in_dim(tables, row + groups, axis=1, keepdims=False)
    owner = jnp.arange(owners, dtype=jnp.int32)[:, None]
    source = slot // 2
    place = (lax.axis_index("zh") ^ (owner % copies)) * 2 + slot % 2
    block = owner * seg_blocks + seg
    codes = (source % near) * slots + place + block * 512
    codes = jnp.where(source // near == lax.axis_index("zh"), codes, -1).reshape(-1)

    todo, count = pl.pallas_call(
        list_kernel,
        out_shape=(
            jax.ShapeDtypeStruct((codes.shape[0] + 2 * TOGETHER,), jnp.int32),
            jax.ShapeDtypeStruct((1,), jnp.int32),
        ),
        in_specs=[SMEM],
        out_specs=[SMEM, SMEM],
        compiler_params=room(1),
    )(codes)
    forces = pl.pallas_call(
        force_kernel,
        out_shape=f32(near, 3, slots, BLK),
        in_specs=[SMEM, SMEM, VMEM, VMEM],
        out_specs=VMEM,
        scratch_shapes=[
            pltpu.VMEM(((near * slots + 1) * 8, BLK), jnp.float32),
            pltpu.VMEM((TOGETHER, 2 * BLK, BLK), jnp.bfloat16),
        ],
        compiler_params=room(20),
    )(todo, count, geometry, received.reshape(near * 6 * slots, BLK))
    back = lax.all_to_all(
        forces.reshape(near, 3 * slots, BLK), NEAR, split_axis=0, concat_axis=0, tiled=True
    )
    out = pl.pallas_call(
        pick_kernel,
        out_shape=f32(3, blocks, BLK),
        in_specs=[VMEM] * 2,
        out_specs=VMEM,
        compiler_params=room(4),
    )(pick, back.reshape(near, 3, slots, BLK))
    return jnp.transpose(out, (1, 0, 2))


def solution(mesh):
    groups = mesh.shape["grp"]
    split = Mesh(mesh.devices.reshape(groups, COPIES, 16 // COPIES, 4, 2), GRP_DOM)
    placed = (
        P(GRP_DOM, None, None),
        P(GRP_DOM),
        P(None, GRP_DOM),
        P(None, GRP_DOM),
        P(GRP_DOM, None, None),
        P(GRP_DOM, None, None),
    )
    return jax.shard_map(contact, mesh=split, in_specs=placed, out_specs=P(GRP_DOM, None, None), check_vma=False)
```

```python
import functools
import math

import jax
import jax.numpy as jnp
from jax import lax
from jax.experimental import pallas as pl
from jax.experimental.pallas import tpu as pltpu
from jax.sharding import Mesh
from jax.sharding import PartitionSpec as P


BLK = 128
COPIES = 4
TIME_STEP = 0.5
STIFFNESS = 0.5
RADIUS_SQ = 0.5
SCALE = math.sqrt(math.log2(math.e) / RADIUS_SQ)
GRP_DOM = ("grp", "zh", "zl", "y", "core")
NEAR = ("zl", "y", "core")
VMEM = pl.BlockSpec(memory_space=pltpu.VMEM)
SMEM = pl.BlockSpec(memory_space=pltpu.SMEM)
TOGETHER = 16
NOBODY = 256


def room(mib):
    return pltpu.CompilerParams(vmem_limit_bytes=mib << 20)


def lane_pick(row, index):
    return jnp.take_along_axis(row, index, axis=1, mode="promise_in_bounds")


def geometry_rows(nodes_ref, conn_ref, seg_ref, slot_ref, out_ref):
    blocks = conn_ref.shape[1] // BLK
    parts = nodes_ref.shape[1] // BLK
    index = [
        jnp.concatenate([conn_ref[k : k + 1, b * BLK : (b + 1) * BLK] for b in range(blocks)], axis=0)
        for k in range(3)
    ]
    lanes = [i & (BLK - 1) for i in index]
    part = [i >> 7 for i in index]
    corner = [[None] * 6 for _ in range(3)]
    for comp in range(6):
        for p in range(parts):
            row = jnp.broadcast_to(nodes_ref[comp : comp + 1, p * BLK : (p + 1) * BLK], (blocks, BLK))
            for k in range(3):
                got = lane_pick(row, lanes[k])
                corner[k][comp] = got if p == 0 else jnp.where(part[k] == p, got, corner[k][comp])
    a, b, c = corner
    e = [b[i] - a[i] for i in range(3)]
    f = [c[i] - a[i] for i in range(3)]
    n = [
        0.5 * (e[1] * f[2] - e[2] * f[1]),
        0.5 * (e[2] * f[0] - e[0] * f[2]),
        0.5 * (e[0] * f[1] - e[1] * f[0]),
    ]
    m = [(a[i] + b[i] + c[i]) / 3.0 for i in range(3)]
    u = [(a[i] + b[i] + c[i]) / 3.0 for i in range(3, 6)]
    s = sum(n[i] * (m[i] + TIME_STEP * u[i]) for i in range(3))
    rows = [m[i] * (2.0 * SCALE) for i in range(3)] + [-v for v in n] + [s]
    groups, each = slot_ref.shape[1:]
    tables = jnp.concatenate([slot_ref[0], seg_ref[0]], axis=0).astype(jnp.float32)
    tables = jnp.concatenate([tables, jnp.zeros((2 * groups, BLK - each), jnp.float32)], axis=1)
    for i, row in enumerate(rows + [tables]):
        out_ref[:, i, :] = row


def three_parts(x):
    high = x.astype(jnp.bfloat16)
    rest = x - high.astype(jnp.float32)
    mid = rest.astype(jnp.bfloat16)
    low = (rest - mid.astype(jnp.float32)).astype(jnp.bfloat16)
    return high, mid, low


def exact_dot(onehot, x):
    return sum(jnp.dot(onehot, part, preferred_element_type=jnp.float32) for part in three_parts(x))


def start_kernel(
    copies, near, dest_ref, nodes_ref, corners_ref, conn_ref, seg_ref, slot_ref, out_ref, pick_ref, geo_ref
):
    geometry_rows(corners_ref, conn_ref, seg_ref, slot_ref, geo_ref)
    blocks = dest_ref.shape[1]
    slots = near * copies * 2
    across = jnp.broadcast_to(dest_ref[...].astype(jnp.float32), (blocks, blocks))
    down = across.T
    i = lax.broadcasted_iota(jnp.int32, (blocks, blocks), 0)
    j = lax.broadcasted_iota(jnp.int32, (blocks, blocks), 1)
    same = across == down

    def slot_of(dest, rank):
        dest = dest.astype(jnp.int32)
        return ((dest & (near - 1)) * copies + lax.div(dest, near)) * 2 + rank.astype(jnp.int32)

    rank_row = jnp.sum(jnp.where(same & (i < j), 1.0, 0.0), axis=0, keepdims=True)
    slot_row = slot_of(dest_ref[...], rank_row)
    onehot = (lax.broadcasted_iota(jnp.int32, (slots, blocks), 0) == slot_row).astype(jnp.float32).astype(jnp.bfloat16)
    rank_col = jnp.sum(jnp.where(same & (j < i), 1.0, 0.0), axis=1, keepdims=True)
    slot_col = slot_of(down[:, 0:1], rank_col)
    pick_ref[...] = (
        (lax.broadcasted_iota(jnp.int32, (blocks, slots), 1) == slot_col).astype(jnp.float32).astype(jnp.bfloat16)
    )
    for comp in range(6):
        x = nodes_ref[comp % 3]
        row = x * SCALE if comp < 3 else x + TIME_STEP * nodes_ref[comp]
        out_ref[:, comp] = exact_dot(onehot, row).reshape(near, copies * 2, BLK)


def split_two(x):
    high = x.astype(jnp.bfloat16).astype(jnp.float32)
    return high, x - high


def split_three(x):
    high, rest = split_two(x)
    mid, low = split_two(rest)
    return high, mid, low


def list_kernel(codes_ref, todo_ref):
    def keep(k, count):
        code = codes_ref[k]
        todo_ref[count] = code
        return count + 1 + (code >> 31)

    count = lax.fori_loop(0, codes_ref.shape[0], keep, jnp.int32(0), unroll=64)
    for k in range(2 * TOGETHER):
        todo_ref[count + k] = NOBODY
    todo_ref[todo_ref.shape[0] - 1] = count


def force_kernel(todo_ref, geo_ref, nodes_ref, out_ref, total, press):
    near, _, slots, _ = out_ref.shape
    total[...] = jnp.zeros_like(total)
    row = lax.broadcasted_iota(jnp.int32, (8, BLK), 0)
    is_close = (row >= 3) & (row < 7)
    is_far = (row < 3) | (row == 7)
    zero = jnp.zeros((8, BLK), jnp.float32)
    minus = jnp.full((8, BLK), -1.0, jnp.float32)

    def geometry(code):
        return geo_ref[pl.ds(pl.multiple_of((code >> 9) * 8, 8), 8), :]

    def begin(k):
        for n in range(TOGETHER):
            code = todo_ref[k * TOGETHER + n]
            tile = geometry(code)
            square = jnp.sum(jnp.where(row < 3, tile * tile, 0.0), axis=0, keepdims=True) * -0.25
            high, mid, low = split_three(jnp.where(row == 7, square, tile))
            left = jnp.concatenate([high, high, high, mid, mid, low, minus, zero], axis=0)
            left = left.astype(jnp.bfloat16).T

            slot = code & 511
            source = jnp.minimum(lax.div(slot, slots), near - 1)
            start = source * (6 * slots) + lax.rem(slot, slots)
            tile = nodes_ref[pl.ds(start, 6, stride=slots), :]
            square = jnp.sum(tile[0:3] * tile[0:3], axis=0, keepdims=True)
            high, mid, low = split_three(
                jnp.concatenate([tile, jnp.ones((2, BLK), jnp.float32)], axis=0)
            )
            order = [high, mid, low, high, mid, high]
            close = [jnp.where(is_close, part, 0.0) for part in order] + [zero, zero]
            high, mid, low = split_three(square)
            last = jnp.where(row == 0, high, jnp.where(row == 1, mid, jnp.where(row == 2, low, 0.0)))
            far = [jnp.where(is_far, part, 0.0) for part in order] + [last, zero]
            right = jnp.concatenate(
                [
                    jnp.concatenate(close, axis=0).astype(jnp.bfloat16),
                    jnp.concatenate(far, axis=0).astype(jnp.bfloat16),
                ],
                axis=1,
            )
            both = jnp.dot(left, right, preferred_element_type=jnp.float32)
            pressure = jnp.exp2(both[:, BLK:]) * jnp.maximum(both[:, :BLK], 0.0)
            high = pressure.astype(jnp.bfloat16)
            press[n, 0:BLK] = high
            press[n, BLK:] = (pressure - high.astype(jnp.float32)).astype(jnp.bfloat16)

    def finish(k):
        for n in range(TOGETHER):
            code = todo_ref[k * TOGETHER + n]
            normal = jnp.concatenate(split_two(geometry(code)), axis=0).astype(jnp.bfloat16)
            normal = jnp.concatenate([normal, normal], axis=1)
            force = jnp.dot(normal, press[n], preferred_element_type=jnp.float32)
            at = pl.ds(pl.multiple_of((code & 511) * 8, 8), 8)
            total[at, :] = total[at, :] + (force[0:8] + force[8:16])

    def step(k, _):
        finish(k)
        begin(k + 1)
        return 0

    last = jnp.maximum(lax.div(todo_ref[todo_ref.shape[0] - 1] + (TOGETHER - 1), TOGETHER) - 1, 0)
    begin(0)
    lax.fori_loop(0, last, step, 0)
    finish(last)
    for source in range(near):
        for comp in range(3):
            for half in range(slots // 8):
                out_ref[source, comp, half * 8 : half * 8 + 8, :] = total[
                    pl.ds((source * slots + half * 8) * 8 + 3 + comp, 8, stride=8), :
                ]


def pick_kernel(pick_ref, back_ref, out_ref):
    for comp in range(3):
        rows = back_ref[:, comp].reshape(pick_ref.shape[1], BLK)
        out_ref[comp] = -STIFFNESS * exact_dot(pick_ref[...], rows)


def f32(*shape):
    return jax.ShapeDtypeStruct(shape, jnp.float32)


def contact(node_state, node_dest, seg_nodes, seg_conn, pair_seg, pair_slot):
    groups = lax.axis_size("grp")
    copies = lax.axis_size("zh")
    near = lax.axis_size(NEAR)
    blocks = node_state.shape[0]
    seg_blocks = seg_conn.shape[1] // BLK
    per_group = pair_seg.shape[2]
    slots = copies * 2
    owners = groups * copies

    outgoing, pick, geometry = pl.pallas_call(
        functools.partial(start_kernel, copies, near),
        out_shape=(
            f32(near, 6, slots, BLK),
            jax.ShapeDtypeStruct((blocks, near * slots), jnp.bfloat16),
            f32(seg_blocks, 8, BLK),
        ),
        in_specs=[VMEM] * 6,
        out_specs=[VMEM] * 3,
    )(
        node_dest.reshape(1, blocks),
        jnp.transpose(node_state, (1, 0, 2)),
        seg_nodes,
        seg_conn,
        pair_seg,
        pair_slot,
    )
    geometry = geometry.reshape(seg_blocks * 8, BLK)
    pieces = [geometry]
    for other in range(1, copies):
        pieces.append(lax.ppermute(geometry, "zh", [(i, i ^ other) for i in range(copies)]))
    received = lax.all_to_all(
        outgoing.reshape(near, 6 * slots, BLK), NEAR, split_axis=0, concat_axis=0, tiled=True
    )
    geometry = lax.all_gather(jnp.concatenate(pieces, axis=0), "grp", axis=0, tiled=True)

    tables = geometry.reshape(owners, seg_blocks, 8, BLK)[:, :, 7, :per_group].astype(jnp.int32)
    row = lax.axis_index("grp")
    slot = lax.dynamic_index_in_dim(tables, row, axis=1, keepdims=False)
    seg = lax.dynamic_index_in_dim(tables, row + groups, axis=1, keepdims=False)
    owner = jnp.arange(owners, dtype=jnp.int32)[:, None]
    source = slot // 2
    place = (lax.axis_index("zh") ^ (owner % copies)) * 2 + slot % 2
    block = owner * seg_blocks + seg
    codes = (source % near) * slots + place + block * 512
    codes = jnp.where(source // near == lax.axis_index("zh"), codes, -1).reshape(-1)

    todo = pl.pallas_call(
        list_kernel,
        out_shape=jax.ShapeDtypeStruct((codes.shape[0] + 2 * TOGETHER + 1,), jnp.int32),
        in_specs=[SMEM],
        out_specs=SMEM,
        compiler_params=room(1),
    )(codes)
    forces = pl.pallas_call(
        force_kernel,
        out_shape=f32(near, 3, slots, BLK),
        in_specs=[SMEM, VMEM, VMEM],
        out_specs=VMEM,
        scratch_shapes=[
            pltpu.VMEM(((near * slots + 1) * 8, BLK), jnp.float32),
            pltpu.VMEM((TOGETHER, 2 * BLK, BLK), jnp.bfloat16),
        ],
        compiler_params=room(20),
    )(todo, geometry, received.reshape(near * 6 * slots, BLK))
    back = lax.all_to_all(
        forces.reshape(near, 3 * slots, BLK), NEAR, split_axis=0, concat_axis=0, tiled=True
    )
    out = pl.pallas_call(
        pick_kernel,
        out_shape=f32(3, blocks, BLK),
        in_specs=[VMEM] * 2,
        out_specs=VMEM,
        compiler_params=room(4),
    )(pick, back.reshape(near, 3, slots, BLK))
    return jnp.transpose(out, (1, 0, 2))


def solution(mesh):
    groups = mesh.shape["grp"]
    split = Mesh(mesh.devices.reshape(groups, COPIES, 16 // COPIES, 4, 2), GRP_DOM)
    placed = (
        P(GRP_DOM, None, None),
        P(GRP_DOM),
        P(None, GRP_DOM),
        P(None, GRP_DOM),
        P(GRP_DOM, None, None),
        P(GRP_DOM, None, None),
    )
    return jax.shard_map(contact, mesh=split, in_specs=placed, out_specs=P(GRP_DOM, None, None), check_vma=False)
```
